128 devices in a mesh: slab: 16 (over y, x), lev: 8 (over z, core).
Axes of the slice: x: 4, y: 4, z: 4, core: 2. Of those that a mesh axis runs over, the one named last changes fastest.
Arguments:
- ensemble: float32 [80, 32, 36864], P(None, 'lev', 'slab'), may hold values from -6 to 6
- obs_cell: int32 [2, 256], replicated, may hold values from 0 to 1179647, as said below
- obs_value: float32 [2, 256], replicated, may hold values from -6 to 6
- obs_var: float32 [2, 256], replicated, may hold values from 0.3 to 3
- obs_frac: float32 [2, 256], replicated, may hold values from 0 to 1
- loc_column: bfloat16 [2, 256, 36864], P(None, 'lev', 'slab'), may hold values from 0 to 1
- loc_level: float32 [2, 256, 32], P(None, None, 'lev'), may hold values from 0.2 to 1
Outputs:
- analysis: float32 [80, 32, 36864], P(None, 'lev', 'slab')
- prior_mean: float32 [2, 256], replicated
The draws below stay inside these ranges and needn't reach their ends.
Inputs may be any that keep to these rules, and one draw needn't show every extreme that they name: `obs_cell`: in each block, every device's cells (a level band of 4 levels and a slab of 2304 columns) hold at least one observation, and one of them lies in the slab's last column.
All inputs are finite; a program needn't handle non-finite values.
Results may differ from the reference program's by a relative error of at most 0.0055.
Values may be sent and summed in bfloat16 or wider, within the bound.
A program may use at most 64 MiB of HBM per device.

```python
import math
import jax
import jax.numpy as jnp
from jax import lax

MEM = 80
CL = 4
CC = 2304
NOBS = 256
BLOCKS = 2
NL = 32
NC = 36864


def draw_obs_cell(key, part):
    n_slabs = NC // CC
    n_bands = NL // CL
    owners = n_slabs * n_bands
    block_rows = []
    for block_index in range(BLOCKS):
        block_key = jax.random.fold_in(key, 101 + block_index)
        keys = jax.random.split(block_key, 6)
        owner_ids = jax.random.permutation(keys[0], owners).astype(jnp.int32)
        owner_slab = owner_ids % n_slabs
        owner_band = owner_ids // n_slabs
        owner_level = owner_band * CL + jax.random.randint(keys[1], (owners,), 0, CL, dtype=jnp.int32)
        owner_column = owner_slab * CC + CC - 1
        extra = NOBS - owners
        rest_level = jax.random.randint(keys[2], (extra,), 0, NL, dtype=jnp.int32)
        slab_one = jax.random.randint(keys[3], (extra,), 0, n_slabs, dtype=jnp.int32)
        slab_two = jax.random.randint(keys[4], (extra,), 0, n_slabs, dtype=jnp.int32)
        rest_slab = slab_one * slab_two // n_slabs
        rest_column = rest_slab * CC + jax.random.randint(keys[5], (extra,), 0, CC, dtype=jnp.int32)
        levels_all = jnp.concatenate([owner_level, rest_level])
        columns_all = jnp.concatenate([owner_column, rest_column])
        block_rows.append((levels_all * NC + columns_all).astype(jnp.int32))
    return jnp.stack(block_rows)


def steps_of(own_key, dims, cuts, smallest, largest):
    def one(position, shards_of):
        steps = jax.random.uniform(jax.random.fold_in(jax.random.fold_in(own_key, 6), position), (shards_of,), jnp.float32, smallest / len(cuts), largest / len(cuts))
        return jnp.repeat(jnp.exp(steps), dims[position] // shards_of).reshape((-1,) + (1,) * (len(dims) - position - 1))

    factor_of = one(*cuts[0])
    for cut in cuts[1:]:
        factor_of = factor_of * one(*cut)
    return factor_of


def scatter_about(key, shape, scale, reach, cuts=(), kind=jnp.bfloat16):
    gain = steps_of(key, shape, cuts, -0.22, 0.18) if cuts else 1.0
    array = jax.random.normal(key, shape, jnp.float32) * scale * gain
    return jnp.minimum(jnp.maximum(array, -reach), reach).astype(kind)


def setup_inputs(seed: int = 0) -> dict:
    seeds = jax.random.split(jax.random.key(seed), 8)
    ensemble = scatter_about(seeds[0], (MEM, NL, NC), 1.0, 6.0, ((1, 8), (2, 16)), jnp.float32)
    obs_cell = draw_obs_cell(jax.random.fold_in(seeds[7], 71), 0)
    obs_value = scatter_about(seeds[2], (BLOCKS, NOBS), 1.5, 6.0, (), jnp.float32)
    obs_var = jnp.clip(jnp.exp(jax.random.uniform(seeds[3], (BLOCKS, NOBS), jnp.float32, math.log(0.3), math.log(3.0))), 0.3, 3.0)
    obs_frac = jnp.clip(jax.random.uniform(seeds[4], (BLOCKS, NOBS), jnp.float32, 0.0, 1.0), 0.0, 1.0)
    loc_column = jnp.clip(1.0 * jax.random.uniform(seeds[5], (BLOCKS, NOBS, NC), jnp.float32) ** steps_of(seeds[5], (BLOCKS, NOBS, NC), ((1, 8), (2, 16)), -0.2, 0.2), 0.0, 1.0).astype(jnp.bfloat16)
    loc_level = jnp.clip(0.2 + 0.8 * jax.random.uniform(seeds[6], (BLOCKS, NOBS, NL), jnp.float32) ** steps_of(seeds[6], (BLOCKS, NOBS, NL), ((2, 8),), -0.2, 0.2), 0.2, 1.0)
    return dict(ensemble=ensemble, obs_cell=obs_cell, obs_value=obs_value, obs_var=obs_var, obs_frac=obs_frac, loc_column=loc_column, loc_level=loc_level)


def obs_stats(prior_obs, obs_val, variance):
    members = prior_obs.shape[1]
    obs_mean = lax.optimization_barrier(jnp.mean(prior_obs, axis=1))
    deviation = prior_obs - obs_mean[:, None]
    spread = lax.optimization_barrier(jnp.sum(deviation * deviation, axis=1)) / (members - 1.0)
    total_var = spread + variance
    shrink = 1.0 / (1.0 + jnp.sqrt(variance / total_var))
    gain_rows = ((obs_val - obs_mean)[:, None] - deviation * shrink[:, None]) / (total_var * (members - 1.0))[:, None]
    return (obs_mean, deviation.astype(jnp.bfloat16), gain_rows.astype(jnp.bfloat16))

def reference(ensemble, obs_cell, obs_value, obs_var, obs_frac, loc_column, loc_level):
    current = ensemble
    prior_means = []
    for block_index in range(BLOCKS):
        obs_cells = obs_cell[block_index]
        obs_level = obs_cells // NC
        obs_column = obs_cells % NC
        next_column = (obs_column + 1) % NC
        flattened = current.reshape(MEM, NL * NC)
        first_val = jnp.take(flattened, obs_level * NC + obs_column, axis=1)
        second = jnp.take(flattened, obs_level * NC + next_column, axis=1)
        fraction = obs_frac[block_index]
        prior_obs = ((1.0 - fraction)[None, :] * first_val + fraction[None, :] * second).T
        obs_mean, dev_b, gain_b = obs_stats(prior_obs, obs_value[block_index], obs_var[block_index])
        prior_means.append(obs_mean)
        centred = (current - lax.optimization_barrier(jnp.mean(current, axis=0))).astype(jnp.bfloat16)
        col_weights = loc_column[block_index]
        lev_weights = loc_level[block_index]

        def level_step(level_index):
            level_slab = lax.dynamic_index_in_dim(centred, level_index, 1, keepdims=False)
            level_loc = lax.dynamic_index_in_dim(lev_weights, level_index, 1, keepdims=False)
            cross_cov = jnp.dot(dev_b, level_slab, preferred_element_type=jnp.float32)
            mixed_rows = (level_loc[:, None] * col_weights.astype(jnp.float32) * cross_cov).astype(jnp.bfloat16)
            return jnp.dot(gain_b.T, mixed_rows, preferred_element_type=jnp.float32)
        increment = lax.map(level_step, jnp.arange(NL, dtype=jnp.int32))
        current = current + jnp.transpose(increment, (1, 0, 2))
    return (current, jnp.stack(prior_means))
```

```python
import functools

import jax
import jax.numpy as jnp
from jax import lax
from jax.experimental import pallas as pl
from jax.experimental.pallas import tpu as pltpu
from jax.sharding import PartitionSpec as P

MESH = pl.DeviceIdType.MESH
SLOTS = 64
F32 = jnp.float32
BF16 = jnp.bfloat16


def nt_dot(a, b):
    return lax.dot_general(a, b, (((1,), (1,)), ((), ())), preferred_element_type=F32)


def count_at_least(x, step, number):
    total = jnp.zeros_like(x)
    for k in range(1, number):
        total = total + jnp.where(x >= float(k * step), 1.0, 0.0)
    return total


def split3(x):
    high = x.astype(BF16)
    rest = x - high.astype(F32)
    mid = rest.astype(BF16)
    low = (rest - mid.astype(F32)).astype(BF16)
    return high, mid, low


def exchange_kernel(
    chunks, n_slab, n_lev,
    cell_ref, value_ref, var_ref, frac_ref, level_ref, ens_hbm, loc_hbm,
    loc_out, dev_out, gain_out, mean_out,
    ens, loc, abuf, bbuf, acc,
    ens_sem, own_sem, out_sem, a_send, a_recv, b_send, b_recv, l_send, l_recv,
):
    slab = lax.axis_index("slab")
    lev = lax.axis_index("lev")
    lev_rows, members, cols = ens.shape
    n_obs = cell_ref.shape[1]
    total_cols = cols * n_slab
    half = members // 2

    barrier = pltpu.get_barrier_semaphore()
    slab_peer = [lax.rem(slab + k, n_slab) for k in range(n_slab)]
    lev_peer = [lax.rem(lev + k, n_lev) for k in range(n_lev)]
    for k in range(1, n_lev):
        pl.semaphore_signal(barrier, inc=1, device_id=(slab, lev_peer[k]), device_id_type=MESH)
    for k in range(1, n_slab):
        pl.semaphore_signal(barrier, inc=1, device_id=(slab_peer[k], lev), device_id_type=MESH)
    own_copies = [
        pltpu.make_async_copy(loc_hbm.at[b], loc.at[b, lev], own_sem.at[b]) for b in range(2)
    ]
    for copy in own_copies:
        copy.start()
    ens_copies = [
        pltpu.make_async_copy(ens_hbm.at[:, l, :], ens.at[l], ens_sem.at[l])
        for l in range(lev_rows)
    ]
    for copy in ens_copies:
        copy.start()

    slab_f = slab.astype(F32)
    lev_f = lev.astype(F32)
    rows = []
    for b in range(2):
        cell = cell_ref[pl.ds(b, 1), :].astype(F32)
        level = count_at_least(cell, total_cols, n_lev * lev_rows)
        column = cell - level * float(total_cols)
        later = column + 1.0
        later = jnp.where(later >= float(total_cols), 0.0, later)
        band = count_at_least(level, lev_rows, n_lev)
        inner = level - band * float(lev_rows)
        places = []
        for where_at in (column, later):
            in_slab = count_at_least(where_at, cols, n_slab)
            place = where_at - in_slab * float(cols) + 1.0
            places.append(jnp.where(in_slab == slab_f, place, 0.0))
        rows.append(
            [band, places[0], places[1], inner,
             value_ref[pl.ds(b, 1), :], var_ref[pl.ds(b, 1), :], frac_ref[pl.ds(b, 1), :]]
        )
    flat = rows[0] + rows[1]
    table = jnp.concatenate(flat + [jnp.zeros((128 - len(flat), n_obs), F32)], axis=0).T

    def column_of(b, i):
        return table[:, 7 * b + i : 7 * b + i + 1]

    lane = lax.broadcasted_iota(jnp.int32, (n_obs, 128), 1)
    lane_slot = jnp.where(lane < SLOTS, lane, lane - SLOTS).astype(F32)
    first_half = lane < SLOTS
    ranks = []
    slot_info = []
    for b in range(2):
        other = lax.broadcasted_iota(jnp.int32, (n_obs, n_obs), 1)
        mine = lax.broadcasted_iota(jnp.int32, (n_obs, n_obs), 0)
        earlier = (column_of(b, 0) == rows[b][0]) & (other < mine)
        rank = jnp.sum(jnp.where(earlier, 1.0, 0.0), axis=1, keepdims=True)
        ranks.append(rank)
        per_chunk = []
        for q in range(chunks):
            chosen = (column_of(b, 0) == lev_f) & (rank == lane_slot + float(SLOTS * q))

            def picked(x):
                return jnp.sum(jnp.where(chosen, x, 0.0), axis=0, keepdims=True)

            filled = picked(jnp.ones((n_obs, 128), F32))
            place = picked(jnp.where(first_half, column_of(b, 1), column_of(b, 2))) - 1.0
            inner = picked(jnp.broadcast_to(column_of(b, 3), (n_obs, 128)))
            value = picked(jnp.broadcast_to(column_of(b, 4), (n_obs, 128)))
            var = picked(jnp.broadcast_to(column_of(b, 5), (n_obs, 128))) + (1.0 - filled)
            frac = column_of(b, 6)
            weight = picked(jnp.where(first_half, 1.0 - frac, frac))
            per_chunk.append((place, inner, value, var, weight))
        slot_info.append(per_chunk)

    def loc_copy(b, which, holder, start, count, target):
        piece = loc.at[b, holder, pl.ds(start, count)]
        return pltpu.make_async_remote_copy(
            src_ref=piece, dst_ref=piece,
            send_sem=l_send.at[b, which], recv_sem=l_recv.at[b, which],
            device_id=(slab, target), device_id_type=MESH,
        )

    up = lax.rem(lev + 2, n_lev)
    down = lax.rem(lev + n_lev - 2, n_lev)
    far = lax.rem(lev + 4, n_lev)
    mate = lev + 1 - 2 * lax.rem(lev, 2)
    held = loc.shape[2]
    part = held // 2
    ring = []
    for b in range(2):
        ring.append([
            loc_copy(b, 0, lev, 0, part, up),
            loc_copy(b, 1, lev, part, part, down),
            loc_copy(b, 2, lev, part, part, up),
            loc_copy(b, 3, lev, 0, part, down),
            loc_copy(b, 4, down, 0, part, up),
            loc_copy(b, 5, up, part, part, down),
            loc_copy(b, 6, lev, 0, held, mate),
            loc_copy(b, 7, down, 0, held, mate),
            loc_copy(b, 8, up, 0, held, mate),
            loc_copy(b, 9, far, 0, held, mate),
        ])

    def ring_begin(b):
        for i in (0, 1, 2, 3, 6):
            ring[b][i].start()

    def ring_forward(b):
        ring[b][0].wait_recv()
        ring[b][4].start()
        ring[b][1].wait_recv()
        ring[b][5].start()
        ring[b][2].wait_recv()
        ring[b][7].start()
        ring[b][3].wait_recv()
        ring[b][8].start()

    def ring_finish(b):
        ring[b][4].wait_recv()
        ring[b][5].wait_recv()
        ring[b][9].start()
        for i in (6, 7, 8, 9):
            ring[b][i].wait_recv()

    def a_copy(r, k):
        return pltpu.make_async_remote_copy(
            src_ref=abuf.at[r, 0], dst_ref=abuf.at[r, k],
            send_sem=a_send.at[r, k], recv_sem=a_recv.at[r, k],
            device_id=(slab_peer[k], lev), device_id_type=MESH,
        )

    def b_copy(r, k):
        return pltpu.make_async_remote_copy(
            src_ref=bbuf.at[r, 0], dst_ref=bbuf.at[r, k],
            send_sem=b_send.at[r, k], recv_sem=b_recv.at[r, k],
            device_id=(slab, lev_peer[k]), device_id_type=MESH,
        )

    lane1 = lax.broadcasted_iota(jnp.int32, (1, 128), 1)
    low1 = lane1 < SLOTS

    def send_priors(r, cells):
        for q in range(chunks):
            weighted = cells[q] * slot_info[r][q][4]
            both = weighted + pltpu.roll(weighted, SLOTS, 1)
            abuf[r, 0, q] = jnp.where(low1, both[:half], both[half:])
        for k in range(1, n_slab):
            a_copy(r, k).start()

    def band_statistics(r):
        for k in range(1, n_slab):
            a_copy(r, k).wait_recv()
        for q in range(chunks):
            packed = abuf[r, 0, q]
            for k in range(1, n_slab):
                packed = packed + abuf[r, k, q]
            turned = pltpu.roll(packed, SLOTS, 1)
            prior = jnp.concatenate(
                [jnp.where(low1, packed, turned), jnp.where(low1, turned, packed)], axis=0
            )
            _, _, value, variance, _ = slot_info[r][q]
            mean = jnp.sum(prior, axis=0, keepdims=True) / float(members)
            deviation = prior - mean
            spread = jnp.sum(deviation * deviation, axis=0, keepdims=True) / (members - 1.0)
            total = spread + variance
            shrink = 1.0 / (1.0 + jnp.sqrt(variance / total))
            gain = ((value - mean) - deviation * shrink) / (total * (members - 1.0))
            bbuf[r, 0, q, pl.ds(0, members), :] = jnp.where(low1, deviation, gain).astype(BF16)
            high, mid, low = (x.astype(F32) for x in split3(mean))
            row = lax.broadcasted_iota(jnp.int32, (16, 128), 0)
            parts = jnp.where(row == 0, high, jnp.where(row == 1, mid, jnp.where(row == 2, low, 0.0)))
            bbuf[r, 0, q, pl.ds(members, 16), :] = parts.astype(BF16)
        for k in range(1, n_lev):
            b_copy(r, k).start()

    def obs_order(r):
        away = lev_f - column_of(r, 0)
        away = jnp.where(away < 0.0, away + float(n_lev), away)
        to_dev = []
        to_gain = []
        for k in range(n_lev):
            for q in range(chunks):
                chosen = (away == float(k)) & (ranks[r] == lane_slot + float(SLOTS * q))
                to_dev.append(jnp.where(chosen & first_half, 1.0, 0.0).astype(BF16))
                to_gain.append(jnp.where(chosen & ~first_half, 1.0, 0.0).astype(BF16))
        return jnp.concatenate(to_dev, axis=1), jnp.concatenate(to_gain, axis=1)

    def all_statistics(r, to_dev, to_gain):
        for k in range(1, n_lev):
            b_copy(r, k).wait_recv()
        packed = jnp.concatenate(
            [bbuf[r, k, q] for k in range(n_lev) for q in range(chunks)], axis=1
        )
        dev = nt_dot(to_dev, packed)[:, :members].astype(BF16)
        gain = nt_dot(packed[:members], to_gain).astype(BF16)
        means = nt_dot(packed[members:], to_dev)
        dev_out[r] = dev
        gain_out[r] = gain
        mean_out[pl.ds(r, 1), :] = means[0:1] + means[1:2] + means[2:3]
        return dev, gain

    wide = 256 * chunks
    places = jnp.concatenate(
        [slot_info[b][q][0] for b in range(2) for q in range(chunks)], axis=1
    )
    inners = jnp.concatenate(
        [slot_info[b][q][1] for b in range(2) for q in range(chunks)], axis=1
    )
    at_level = [jnp.where(inners == float(l), places, -1.0) for l in range(lev_rows)]
    acc[...] = jnp.zeros_like(acc)

    pl.semaphore_wait(barrier, n_lev + n_slab - 2)
    own_copies[0].wait()
    ring_begin(0)
    for copy in ens_copies:
        copy.wait()

    step_cols = 256

    def gather_step(c, carry):
        base = c * step_cols
        here = pl.ds(pl.multiple_of(base, step_cols), step_cols)
        index = (lax.broadcasted_iota(jnp.int32, (step_cols, wide), 0) + base).astype(F32)
        hot = jnp.concatenate(
            [jnp.where(index == at_level[l], 1.0, 0.0).astype(BF16) for l in range(lev_rows)],
            axis=0,
        )
        pieces = [split3(ens[l, :, here]) for l in range(lev_rows)]
        left = jnp.concatenate(
            [jnp.concatenate([pieces[l][i] for l in range(lev_rows)], axis=1) for i in range(3)],
            axis=0,
        )
        acc[...] += jnp.dot(left, hot, preferred_element_type=F32)
        return carry

    lax.fori_loop(0, cols // step_cols, gather_step, 0)
    picked_cells = acc[:members] + acc[members : 2 * members] + acc[2 * members :]
    cells = [
        [picked_cells[:, 128 * (b * chunks + q) : 128 * (b * chunks + q + 1)] for q in range(chunks)]
        for b in range(2)
    ]

    send_priors(0, cells[0])
    ring_forward(0)
    own_copies[1].wait()
    to_dev, to_gain = obs_order(0)
    band_statistics(0)
    ring_finish(0)

    later_places = jnp.concatenate([slot_info[1][q][0] for q in range(chunks)], axis=1)
    later_inners = jnp.concatenate([slot_info[1][q][1] for q in range(chunks)], axis=1)
    narrow = 128 * chunks
    index = lax.broadcasted_iota(jnp.int32, (cols, narrow), 0).astype(F32)
    hot = jnp.where(index == later_places, 1.0, 0.0).astype(BF16)
    weights = jnp.dot(loc[0].reshape(n_obs, cols), hot, preferred_element_type=F32)
    level_weight = jnp.zeros((n_obs, narrow), F32)
    for l in range(lev_rows):
        level_weight = jnp.where(later_inners == float(l), level_ref[0, :, l : l + 1], level_weight)
    weights = level_weight * weights

    dev, gain = all_statistics(0, to_dev, to_gain)
    ring_begin(1)
    now = jnp.concatenate(cells[1], axis=1)
    centred = (now - jnp.sum(now, axis=0, keepdims=True) / float(members)).astype(BF16)
    cross = jnp.dot(dev, centred, preferred_element_type=F32)
    mixed = (weights * cross).astype(BF16)
    now = now + jnp.dot(gain, mixed, preferred_element_type=F32)
    send_priors(1, [now[:, 128 * q : 128 * (q + 1)] for q in range(chunks)])

    out_copies = [pltpu.make_async_copy(loc.at[b], loc_out.at[b], out_sem.at[b]) for b in range(2)]
    out_copies[0].start()
    ring_forward(1)
    to_dev, to_gain = obs_order(1)
    band_statistics(1)
    ring_finish(1)
    out_copies[1].start()
    all_statistics(1, to_dev, to_gain)

    for b in range(2):
        for copy in ring[b]:
            copy.wait_send()
        for k in range(1, n_slab):
            a_copy(b, k).wait_send()
        for k in range(1, n_lev):
            b_copy(b, k).wait_send()
    for copy in out_copies:
        copy.wait()


def exchange(chunks, n_slab, n_lev, obs_cell, obs_value, obs_var, obs_frac, loc_level, ensemble, loc_column):
    members, lev_rows, cols = ensemble.shape
    n_obs = obs_cell.shape[1]
    held = loc_column.shape[1]
    vmem = pl.BlockSpec(memory_space=pltpu.VMEM)
    hbm = pl.BlockSpec(memory_space=pl.ANY)
    dma = pltpu.SemaphoreType.DMA
    return pl.pallas_call(
        functools.partial(exchange_kernel, chunks, n_slab, n_lev),
        out_shape=(
            jax.ShapeDtypeStruct((2, n_lev, held, cols), BF16),
            jax.ShapeDtypeStruct((2, n_obs, members), BF16),
            jax.ShapeDtypeStruct((2, members, n_obs), BF16),
            jax.ShapeDtypeStruct((2, n_obs), F32),
        ),
        in_specs=[vmem] * 5 + [hbm] * 2,
        out_specs=(hbm, vmem, vmem, vmem),
        scratch_shapes=[
            pltpu.VMEM((lev_rows, members, cols), F32),
            pltpu.VMEM((2, n_lev, held, cols), BF16),
            pltpu.VMEM((2, n_slab, chunks, members // 2, 128), F32),
            pltpu.VMEM((2, n_lev, chunks, members + 16, 128), BF16),
            pltpu.VMEM((3 * members, 256 * chunks), F32),
            dma((lev_rows,)),
            dma((2,)),
            dma((2,)),
            dma((2, n_slab)),
            dma((2, n_slab)),
            dma((2, n_lev)),
            dma((2, n_lev)),
            dma((2, 10)),
            dma((2, 10)),
        ],
        compiler_params=pltpu.CompilerParams(
            collective_id=chunks, has_side_effects=True, vmem_limit_bytes=60 * 1024 * 1024
        ),
    )(obs_cell, obs_value, obs_var, obs_frac, loc_level, ensemble, loc_column)


def regress_kernel(
    width, dev_ref, gain_ref, level_ref, ens_hbm, loc_hbm, out_hbm,
    ens, out, loc, level, in_sem, loc_sem, out_sem,
):
    lev_rows, members, cols = ens.shape
    n_obs = dev_ref.shape[1]
    steps = cols // width

    def at(c):
        return pl.ds(pl.multiple_of(c * width, width), width)

    def in_copy(c, l):
        return pltpu.make_async_copy(ens_hbm.at[:, l, at(c)], ens.at[l, :, at(c)], in_sem.at[c, l])

    def loc_copy(c, b):
        return pltpu.make_async_copy(loc_hbm.at[b, :, at(c)], loc.at[b, :, at(c)], loc_sem.at[c, b])

    def out_copy(c, l):
        return pltpu.make_async_copy(out.at[l, :, at(c)], out_hbm.at[:, l, at(c)], out_sem.at[c, l])

    for c in range(steps):
        for b in range(2):
            loc_copy(c, b).start()
        for l in range(lev_rows):
            in_copy(c, l).start()
    for b in range(2):
        for l in range(lev_rows):
            level[b, l] = jnp.broadcast_to(level_ref[b, :, l : l + 1], (n_obs, 128))

    def step(c, carry):
        for b in range(2):
            loc_copy(c, b).wait()
        for l in range(lev_rows):
            in_copy(c, l).wait()
        for b in range(2):
            source = ens if b == 0 else out
            local = loc[b, :, at(c)].astype(F32)
            for l in range(lev_rows):
                now = source[l, :, at(c)]
                mean = jnp.sum(now, axis=0, keepdims=True) / float(members)
                centred = (now - mean).astype(BF16)
                cross = jnp.dot(dev_ref[b], centred, preferred_element_type=F32)
                weight = jnp.tile(level[b, l], (1, width // 128)) * local
                mixed = (weight * cross).astype(BF16)
                out[l, :, at(c)] = now + jnp.dot(gain_ref[b], mixed, preferred_element_type=F32)
        for l in range(lev_rows):
            out_copy(c, l).start()
        return carry

    lax.fori_loop(0, steps, step, 0)
    for c in range(steps):
        for l in range(lev_rows):
            out_copy(c, l).wait()


def regress(dev, gain, loc_level, ensemble, loc_all):
    members, lev_rows, cols = ensemble.shape
    n_obs = dev.shape[1]
    width = 768 if cols % 768 == 0 else cols
    vmem = pl.BlockSpec(memory_space=pltpu.VMEM)
    hbm = pl.BlockSpec(memory_space=pl.ANY)
    dma = pltpu.SemaphoreType.DMA
    return pl.pallas_call(
        functools.partial(regress_kernel, width),
        out_shape=jax.ShapeDtypeStruct(ensemble.shape, F32),
        in_specs=[vmem] * 3 + [hbm] * 2,
        out_specs=hbm,
        scratch_shapes=[
            pltpu.VMEM((lev_rows, members, cols), F32),
            pltpu.VMEM((lev_rows, members, cols), F32),
            pltpu.VMEM((2, n_obs, cols), BF16),
            pltpu.VMEM((2, lev_rows, n_obs, 128), F32),
            dma((cols // width, lev_rows)),
            dma((cols // width, 2)),
            dma((cols // width, lev_rows)),
        ],
        compiler_params=pltpu.CompilerParams(vmem_limit_bytes=60 * 1024 * 1024),
    )(dev, gain, loc_level, ensemble, loc_all)


def on_device(n_slab, n_lev, ensemble, obs_cell, obs_value, obs_var, obs_frac, loc_column, loc_level):
    members, lev_rows, slab_cols = ensemble.shape
    n_obs = obs_cell.shape[1]
    band = obs_cell // (slab_cols * n_slab * lev_rows)
    crowd = jnp.sum((band[:, :, None] == jnp.arange(n_lev)).astype(jnp.int32), axis=1)
    operands = (obs_cell, obs_value, obs_var, obs_frac, loc_level, ensemble, loc_column)
    loc_all, dev, gain, prior_mean = lax.cond(
        jnp.max(crowd) <= SLOTS,
        functools.partial(exchange, 1, n_slab, n_lev),
        functools.partial(exchange, 3, n_slab, n_lev),
        *operands,
    )
    analysis = regress(dev, gain, loc_level, ensemble, loc_all.reshape(2, n_obs, slab_cols))
    return analysis, prior_mean


def solution(mesh):
    in_specs = (
        P(None, "lev", "slab"),
        P(),
        P(),
        P(),
        P(),
        P(None, "lev", "slab"),
        P(None, None, "lev"),
    )
    out_specs = (P(None, "lev", "slab"), P())
    return jax.shard_map(
        functools.partial(on_device, mesh.shape["slab"], mesh.shape["lev"]),
        mesh=mesh, in_specs=in_specs, out_specs=out_specs, check_vma=False,
    )
```

```python
import functools

import jax
import jax.numpy as jnp
from jax import lax
from jax.experimental import pallas as pl
from jax.experimental.pallas import tpu as pltpu
from jax.sharding import PartitionSpec as P

MESH = pl.DeviceIdType.MESH
SLOTS = 64
F32 = jnp.float32
BF16 = jnp.bfloat16


def nt_dot(a, b):
    return lax.dot_general(a, b, (((1,), (1,)), ((), ())), preferred_element_type=F32)


def count_at_least(x, step, number):
    total = jnp.zeros_like(x)
    for k in range(1, number):
        total = total + jnp.where(x >= float(k * step), 1.0, 0.0)
    return total


def split3(x):
    high = x.astype(BF16)
    rest = x - high.astype(F32)
    mid = rest.astype(BF16)
    low = (rest - mid.astype(F32)).astype(BF16)
    return high, mid, low


class Tracker:
    def __init__(self):
        self.sends = []
        self.recvs = []

    def start(self, copy):
        copy.start()
        self.sends.append(copy)
        self.recvs.append(copy)

    def arrived(self, copy):
        copy.wait_recv()
        self.recvs = [c for c in self.recvs if c is not copy]

    def drain(self):
        for copy in self.recvs:
            copy.wait_recv()
        for copy in self.sends:
            copy.wait_send()


def filter_kernel(
    chunks, n_slab, n_lev, width,
    cell_hbm, value_hbm, var_hbm, frac_hbm, level_hbm, ens_hbm, loc_hbm,
    ens, loc_last, dev_out, gain_out, level_out, mean_out,
    loc_first, cell_ref, value_ref, var_ref, frac_ref, level_ref, abuf, bbuf, acc, level_wide,
    small_sem, ens_sem, own_sem, a_send, a_recv, b_send, b_recv, l_send, l_recv,
):
    slab = lax.axis_index("slab")
    lev = lax.axis_index("lev")
    lev_rows, members, cols = ens.shape
    n_obs = cell_ref.shape[1]
    loc = (loc_first, loc_last)
    total_cols = cols * n_slab
    half = members // 2
    remote = Tracker()

    barrier = pltpu.get_barrier_semaphore()
    slab_peer = [lax.rem(slab + k, n_slab) for k in range(n_slab)]
    lev_peer = [lax.rem(lev + k, n_lev) for k in range(n_lev)]
    for k in range(1, n_slab):
        pl.semaphore_signal(barrier, inc=1, device_id=(slab_peer[k], lev), device_id_type=MESH)
    for k in range(1, n_lev):
        pl.semaphore_signal(barrier, inc=1, device_id=(slab, lev_peer[k]), device_id_type=MESH)
    small_copies = [
        pltpu.make_async_copy(source, target, small_sem.at[i])
        for i, (source, target) in enumerate([
            (cell_hbm, cell_ref), (value_hbm, value_ref), (var_hbm, var_ref),
            (frac_hbm, frac_ref), (level_hbm, level_ref),
        ])
    ]
    for copy in small_copies:
        copy.start()
    ens_copies = [
        pltpu.make_async_copy(ens_hbm.at[:, l, :], ens.at[l], ens_sem.at[l])
        for l in range(lev_rows)
    ]
    for copy in ens_copies:
        copy.start()
    own_copies = [
        pltpu.make_async_copy(loc_hbm.at[b], loc[b].at[lev], own_sem.at[b]) for b in range(2)
    ]
    for copy in own_copies:
        copy.start()

    for copy in small_copies:
        copy.wait()

    slab_f = slab.astype(F32)
    lev_f = lev.astype(F32)
    rows = []
    for b in range(2):
        cell = cell_ref[pl.ds(b, 1), :].astype(F32)
        level = count_at_least(cell, total_cols, n_lev * lev_rows)
        column = cell - level * float(total_cols)
        later = column + 1.0
        later = jnp.where(later >= float(total_cols), 0.0, later)
        band = count_at_least(level, lev_rows, n_lev)
        inner = level - band * float(lev_rows)
        places = []
        for where_at in (column, later):
            in_slab = count_at_least(where_at, cols, n_slab)
            place = where_at - in_slab * float(cols) + 1.0
            places.append(jnp.where(in_slab == slab_f, place, 0.0))
        rows.append(
            [band, places[0], places[1], inner,
             value_ref[pl.ds(b, 1), :], var_ref[pl.ds(b, 1), :], frac_ref[pl.ds(b, 1), :]]
            + [level_ref[b, pl.ds(l, 1), :] for l in range(lev_rows)]
        )
    per_block = len(rows[0])
    flat = rows[0] + rows[1]
    table = jnp.concatenate(flat + [jnp.zeros((128 - len(flat), n_obs), F32)], axis=0).T

    def column_of(b, i):
        return table[:, per_block * b + i : per_block * b + i + 1]

    lane = lax.broadcasted_iota(jnp.int32, (n_obs, 128), 1)
    lane_slot = jnp.where(lane < SLOTS, lane, lane - SLOTS).astype(F32)
    first_half = lane < SLOTS
    ranks = []
    slot_info = []
    for b in range(2):
        other = lax.broadcasted_iota(jnp.int32, (n_obs, n_obs), 1)
        mine = lax.broadcasted_iota(jnp.int32, (n_obs, n_obs), 0)
        earlier = (column_of(b, 0) == rows[b][0]) & (other < mine)
        rank = jnp.sum(jnp.where(earlier, 1.0, 0.0), axis=1, keepdims=True)
        ranks.append(rank)
        per_chunk = []
        for q in range(chunks):
            chosen = (column_of(b, 0) == lev_f) & (rank == lane_slot + float(SLOTS * q))

            def picked(x):
                return jnp.sum(jnp.where(chosen, x, 0.0), axis=0, keepdims=True)

            filled = picked(jnp.ones((n_obs, 128), F32))
            place = picked(jnp.where(first_half, column_of(b, 1), column_of(b, 2))) - 1.0
            inner = picked(jnp.broadcast_to(column_of(b, 3), (n_obs, 128)))
            value = picked(jnp.broadcast_to(column_of(b, 4), (n_obs, 128)))
            var = picked(jnp.broadcast_to(column_of(b, 5), (n_obs, 128))) + (1.0 - filled)
            frac = column_of(b, 6)
            weight = picked(jnp.where(first_half, 1.0 - frac, frac))
            per_chunk.append((place, inner, value, var, weight))
        slot_info.append(per_chunk)

    def loc_copy(b, which, holder, start, count, target):
        piece = loc[b].at[holder, pl.ds(start, count)]
        return pltpu.make_async_remote_copy(
            src_ref=piece, dst_ref=piece,
            send_sem=l_send.at[b, which], recv_sem=l_recv.at[b, which],
            device_id=(slab, target), device_id_type=MESH,
        )

    up = lax.rem(lev + 2, n_lev)
    down = lax.rem(lev + n_lev - 2, n_lev)
    far = lax.rem(lev + 4, n_lev)
    mate = lev + 1 - 2 * lax.rem(lev, 2)
    held = loc_first.shape[1]
    part = held // 2
    ring = []
    for b in range(2):
        ring.append([
            loc_copy(b, 0, lev, 0, part, up),
            loc_copy(b, 1, lev, part, part, down),
            loc_copy(b, 2, lev, part, part, up),
            loc_copy(b, 3, lev, 0, part, down),
            loc_copy(b, 4, down, 0, part, up),
            loc_copy(b, 5, up, part, part, down),
            loc_copy(b, 6, lev, 0, held, mate),
            loc_copy(b, 7, down, 0, held, mate),
            loc_copy(b, 8, up, 0, held, mate),
            loc_copy(b, 9, far, 0, held, mate),
        ])

    def ring_begin(b):
        for i in (0, 1, 2, 3, 6):
            remote.start(ring[b][i])

    def ring_forward(b):
        for first, then in ((0, 4), (1, 5), (2, 7), (3, 8)):
            remote.arrived(ring[b][first])
            remote.start(ring[b][then])

    def ring_finish(b):
        remote.arrived(ring[b][4])
        remote.arrived(ring[b][5])
        remote.start(ring[b][9])
        for i in (6, 7, 8, 9):
            remote.arrived(ring[b][i])

    a_copies = [[
        pltpu.make_async_remote_copy(
            src_ref=abuf.at[r, 0], dst_ref=abuf.at[r, k],
            send_sem=a_send.at[r, k], recv_sem=a_recv.at[r, k],
            device_id=(slab_peer[k], lev), device_id_type=MESH,
        ) if k else None for k in range(n_slab)] for r in range(2)]
    b_copies = [[
        pltpu.make_async_remote_copy(
            src_ref=bbuf.at[r, 0], dst_ref=bbuf.at[r, k],
            send_sem=b_send.at[r, k], recv_sem=b_recv.at[r, k],
            device_id=(slab, lev_peer[k]), device_id_type=MESH,
        ) if k else None for k in range(n_lev)] for r in range(2)]

    lane1 = lax.broadcasted_iota(jnp.int32, (1, 128), 1)
    low1 = lane1 < SLOTS

    def send_priors(r, cells):
        for q in range(chunks):
            weighted = cells[q] * slot_info[r][q][4]
            both = weighted + pltpu.roll(weighted, SLOTS, 1)
            abuf[r, 0, q] = jnp.where(low1, both[:half], both[half:])
        for k in range(1, n_slab):
            remote.start(a_copies[r][k])

    def band_statistics(r):
        for k in range(1, n_slab):
            remote.arrived(a_copies[r][k])
        for q in range(chunks):
            packed = abuf[r, 0, q]
            for k in range(1, n_slab):
                packed = packed + abuf[r, k, q]
            turned = pltpu.roll(packed, SLOTS, 1)
            prior = jnp.concatenate(
                [jnp.where(low1, packed, turned), jnp.where(low1, turned, packed)], axis=0
            )
            _, _, value, variance, _ = slot_info[r][q]
            mean = jnp.sum(prior, axis=0, keepdims=True) / float(members)
            deviation = prior - mean
            spread = jnp.sum(deviation * deviation, axis=0, keepdims=True) / (members - 1.0)
            total = spread + variance
            shrink = 1.0 / (1.0 + jnp.sqrt(variance / total))
            gain = ((value - mean) - deviation * shrink) / (total * (members - 1.0))
            bbuf[r, 0, q, pl.ds(0, members), :] = jnp.where(low1, deviation, gain).astype(BF16)
            high, mid, low = (x.astype(F32) for x in split3(mean))
            row = lax.broadcasted_iota(jnp.int32, (16, 128), 0)
            parts = jnp.where(row == 0, high, jnp.where(row == 1, mid, jnp.where(row == 2, low, 0.0)))
            bbuf[r, 0, q, pl.ds(members, 16), :] = parts.astype(BF16)
        for k in range(1, n_lev):
            remote.start(b_copies[r][k])

    def obs_order(r):
        away = lev_f - column_of(r, 0)
        away = jnp.where(away < 0.0, away + float(n_lev), away)
        to_dev = []
        to_gain = []
        for k in range(n_lev):
            for q in range(chunks):
                chosen = (away == float(k)) & (ranks[r] == lane_slot + float(SLOTS * q))
                to_dev.append(jnp.where(chosen & first_half, 1.0, 0.0).astype(BF16))
                to_gain.append(jnp.where(chosen & ~first_half, 1.0, 0.0).astype(BF16))
        return jnp.concatenate(to_dev, axis=1), jnp.concatenate(to_gain, axis=1)

    def all_statistics(r, to_dev, to_gain):
        for k in range(1, n_lev):
            remote.arrived(b_copies[r][k])
        packed = jnp.concatenate(
            [bbuf[r, k, q] for k in range(n_lev) for q in range(chunks)], axis=1
        )
        dev = nt_dot(to_dev, packed)[:, :members].astype(BF16)
        gain = nt_dot(packed[:members], to_gain).astype(BF16)
        return dev, gain

    def all_means(r, to_dev):
        packed = jnp.concatenate(
            [bbuf[r, k, q, pl.ds(members, 16), :] for k in range(n_lev) for q in range(chunks)], axis=1
        )
        means = nt_dot(packed, to_dev)
        mean_out[pl.ds(r, 1), :] = means[0:1] + means[1:2] + means[2:3]

    def at(c):
        return pl.ds(pl.multiple_of(c * width, width), width)

    def regress(dev, gain):
        def step(c, carry):
            local = loc_first[:, :, at(c)].reshape(n_obs, width).astype(F32)
            for l in range(lev_rows):
                now = ens[l, :, at(c)]
                mean = jnp.sum(now, axis=0, keepdims=True) / float(members)
                centred = (now - mean).astype(BF16)
                cross = jnp.dot(dev, centred, preferred_element_type=F32)
                weight = jnp.tile(level_wide[l], (1, width // 128)) * local
                mixed = (weight * cross).astype(BF16)
                ens[l, :, at(c)] = now + jnp.dot(gain, mixed, preferred_element_type=F32)
            return carry

        lax.fori_loop(0, cols // width, step, 0)

    wide = 256 * chunks
    places = jnp.concatenate(
        [slot_info[b][q][0] for b in range(2) for q in range(chunks)], axis=1
    )
    inners = jnp.concatenate(
        [slot_info[b][q][1] for b in range(2) for q in range(chunks)], axis=1
    )
    at_level = [jnp.where(inners == float(l), places, -1.0) for l in range(lev_rows)]
    acc[...] = jnp.zeros_like(acc)
    for copy in ens_copies:
        copy.wait()

    step_cols = 256

    def gather_step(c, carry):
        base = c * step_cols
        here = pl.ds(pl.multiple_of(base, step_cols), step_cols)
        index = (lax.broadcasted_iota(jnp.int32, (step_cols, wide), 0) + base).astype(F32)
        hot = jnp.concatenate(
            [jnp.where(index == at_level[l], 1.0, 0.0).astype(BF16) for l in range(lev_rows)],
            axis=0,
        )
        pieces = [split3(ens[l, :, here]) for l in range(lev_rows)]
        left = jnp.concatenate(
            [jnp.concatenate([pieces[l][i] for l in range(lev_rows)], axis=1) for i in range(3)],
            axis=0,
        )
        acc[...] += jnp.dot(left, hot, preferred_element_type=F32)
        return carry

    lax.fori_loop(0, cols // step_cols, gather_step, 0)
    picked_cells = acc[:members] + acc[members : 2 * members] + acc[2 * members :]
    cells = [
        [picked_cells[:, 128 * (b * chunks + q) : 128 * (b * chunks + q + 1)] for q in range(chunks)]
        for b in range(2)
    ]

    pl.semaphore_wait(barrier, n_lev + n_slab - 2)
    send_priors(0, cells[0])
    own_copies[0].wait()
    ring_begin(0)
    to_dev, to_gain = obs_order(0)
    for l in range(lev_rows):
        level_wide[l] = jnp.broadcast_to(column_of(0, 7 + l), (n_obs, 128))
    level_out[...] = table
    ring_forward(0)
    own_copies[1].wait()
    band_statistics(0)
    ring_finish(0)

    later_places = jnp.concatenate([slot_info[1][q][0] for q in range(chunks)], axis=1)
    later_inners = jnp.concatenate([slot_info[1][q][1] for q in range(chunks)], axis=1)
    narrow = 128 * chunks
    index = lax.broadcasted_iota(jnp.int32, (cols, narrow), 0).astype(F32)
    hot = jnp.where(index == later_places, 1.0, 0.0).astype(BF16)
    weights = jnp.dot(loc_first[...].reshape(n_obs, cols), hot, preferred_element_type=F32)
    level_weight = jnp.zeros((n_obs, narrow), F32)
    for l in range(lev_rows):
        level_weight = jnp.where(later_inners == float(l), column_of(0, 7 + l), level_weight)
    weights = level_weight * weights

    dev, gain = all_statistics(0, to_dev, to_gain)
    ring_begin(1)
    now = jnp.concatenate(cells[1], axis=1)
    centred = (now - jnp.sum(now, axis=0, keepdims=True) / float(members)).astype(BF16)
    cross = jnp.dot(dev, centred, preferred_element_type=F32)
    mixed = (weights * cross).astype(BF16)
    now = now + jnp.dot(gain, mixed, preferred_element_type=F32)
    send_priors(1, [now[:, 128 * q : 128 * (q + 1)] for q in range(chunks)])
    all_means(0, to_dev)
    regress(dev, gain)
    ring_forward(1)
    to_dev, to_gain = obs_order(1)
    band_statistics(1)
    ring_finish(1)
    dev, gain = all_statistics(1, to_dev, to_gain)
    dev_out[...] = dev
    gain_out[...] = gain
    all_means(1, to_dev)
    remote.drain()


def run_filter(chunks, n_slab, n_lev, obs_cell, obs_value, obs_var, obs_frac, loc_level, ensemble, loc_column):
    members, lev_rows, cols = ensemble.shape
    n_obs = obs_cell.shape[1]
    held = loc_column.shape[1]
    width = 768 if cols % 768 == 0 else cols
    vmem = pl.BlockSpec(memory_space=pltpu.VMEM)
    hbm = pl.BlockSpec(memory_space=pltpu.HBM)
    dma = pltpu.SemaphoreType.DMA
    return pl.pallas_call(
        functools.partial(filter_kernel, chunks, n_slab, n_lev, width),
        out_shape=(
            jax.ShapeDtypeStruct((lev_rows, members, cols), F32),
            jax.ShapeDtypeStruct((n_lev, held, cols), BF16),
            jax.ShapeDtypeStruct((n_obs, members), BF16),
            jax.ShapeDtypeStruct((members, n_obs), BF16),
            jax.ShapeDtypeStruct((n_obs, 128), F32),
            jax.ShapeDtypeStruct((2, n_obs), F32),
        ),
        in_specs=[hbm] * 7,
        out_specs=(vmem,) * 6,
        scratch_shapes=[
            pltpu.VMEM((n_lev, held, cols), BF16),
            pltpu.VMEM(obs_cell.shape, jnp.int32),
            pltpu.VMEM(obs_cell.shape, F32),
            pltpu.VMEM(obs_cell.shape, F32),
            pltpu.VMEM(obs_cell.shape, F32),
            pltpu.VMEM(loc_level.shape, F32),
            pltpu.VMEM((2, n_slab, chunks, members // 2, 128), F32),
            pltpu.VMEM((2, n_lev, chunks, members + 16, 128), BF16),
            pltpu.VMEM((3 * members, 256 * chunks), F32),
            pltpu.VMEM((lev_rows, n_obs, 128), F32),
            dma((5,)),
            dma((lev_rows,)),
            dma((2,)),
            dma((2, n_slab)),
            dma((2, n_slab)),
            dma((2, n_lev)),
            dma((2, n_lev)),
            dma((2, 10)),
            dma((2, 10)),
        ],
        compiler_params=pltpu.CompilerParams(
            collective_id=chunks, has_side_effects=True, vmem_limit_bytes=VMEM_LIMIT
        ),
    )(obs_cell, obs_value, obs_var, obs_frac, loc_level, ensemble, loc_column)


def last_kernel(width, ens, loc, dev_ref, gain_ref, level_ref, out_hbm, out, out_sem):
    lev_rows, members, cols = ens.shape
    n_obs = dev_ref.shape[0]
    steps = cols // width

    def at(c):
        return pl.ds(pl.multiple_of(c * width, width), width)

    def out_copy(c, l):
        return pltpu.make_async_copy(out.at[l, :, at(c)], out_hbm.at[:, l, at(c)], out_sem.at[c, l])

    dev = dev_ref[...]
    gain = gain_ref[...]

    def step(c, carry):
        local = loc[:, :, at(c)].reshape(n_obs, width).astype(F32)
        for l in range(lev_rows):
            now = ens[l, :, at(c)]
            mean = jnp.sum(now, axis=0, keepdims=True) / float(members)
            centred = (now - mean).astype(BF16)
            cross = jnp.dot(dev, centred, preferred_element_type=F32)
            place = LEVEL_AT + l
            mixed = (level_ref[:, place : place + 1] * local * cross).astype(BF16)
            out[l, :, at(c)] = now + jnp.dot(gain, mixed, preferred_element_type=F32)
            out_copy(c, l).start()
        return carry

    lax.fori_loop(0, steps, step, 0)
    for c in range(steps):
        for l in range(lev_rows):
            out_copy(c, l).wait()


LEVEL_AT = 18
VMEM_LIMIT = 40 * 1024 * 1024
COND = True


def last_update(ens, loc, dev, gain, level):
    lev_rows, members, cols = ens.shape
    width = 768 if cols % 768 == 0 else cols
    vmem = pl.BlockSpec(memory_space=pltpu.VMEM)
    return pl.pallas_call(
        functools.partial(last_kernel, width),
        out_shape=jax.ShapeDtypeStruct((members, lev_rows, cols), F32),
        in_specs=[vmem] * 5,
        out_specs=pl.BlockSpec(memory_space=pl.ANY),
        scratch_shapes=[
            pltpu.VMEM((lev_rows, members, cols), F32),
            pltpu.SemaphoreType.DMA((cols // width, lev_rows)),
        ],
        compiler_params=pltpu.CompilerParams(vmem_limit_bytes=VMEM_LIMIT),
    )(ens, loc, dev, gain, level)


def on_device(n_slab, n_lev, ensemble, obs_cell, obs_value, obs_var, obs_frac, loc_column, loc_level):
    members, lev_rows, slab_cols = ensemble.shape
    n_obs = obs_cell.shape[1]
    operands = (obs_cell, obs_value, obs_var, obs_frac, jnp.swapaxes(loc_level, 1, 2), ensemble, loc_column)
    if COND:
        band_cells = slab_cols * n_slab * lev_rows
        starts = jnp.arange(n_lev, dtype=jnp.int32) * band_cells
        cell = obs_cell[:, :, None]
        inside = (cell >= starts) & (cell < starts + band_cells)
        crowd = jnp.max(jnp.sum(inside.astype(jnp.int32), axis=1))
        state = lax.cond(
            crowd <= SLOTS,
            functools.partial(run_filter, 1, n_slab, n_lev),
            functools.partial(run_filter, 3, n_slab, n_lev),
            *operands,
        )
    else:
        state = run_filter(1, n_slab, n_lev, *operands)
    return last_update(*state[:5]), state[5]


def solution(mesh):
    in_specs = (
        P(None, "lev", "slab"),
        P(),
        P(),
        P(),
        P(),
        P(None, "lev", "slab"),
        P(None, None, "lev"),
    )
    out_specs = (P(None, "lev", "slab"), P())
    return jax.shard_map(
        functools.partial(on_device, mesh.shape["slab"], mesh.shape["lev"]),
        mesh=mesh, in_specs=in_specs, out_specs=out_specs, check_vma=False,
    )
```

```python
import functools

import jax
import jax.numpy as jnp
from jax import lax
from jax.experimental import pallas as pl
from jax.experimental.pallas import tpu as pltpu
from jax.sharding import PartitionSpec as P

MESH = pl.DeviceIdType.MESH
SLOTS = 64
F32 = jnp.float32
BF16 = jnp.bfloat16


def nt_dot(a, b):
    return lax.dot_general(a, b, (((1,), (1,)), ((), ())), preferred_element_type=F32)


def count_at_least(x, step, number):
    total = jnp.zeros_like(x)
    for k in range(1, number):
        total = total + jnp.where(x >= float(k * step), 1.0, 0.0)
    return total


def split3(x):
    high = x.astype(BF16)
    rest = x - high.astype(F32)
    mid = rest.astype(BF16)
    low = (rest - mid.astype(F32)).astype(BF16)
    return high, mid, low


class Tracker:
    def __init__(self):
        self.sends = []
        self.recvs = []

    def start(self, copy):
        copy.start()
        self.sends.append(copy)
        self.recvs.append(copy)

    def arrived(self, copy):
        copy.wait_recv()
        self.recvs = [c for c in self.recvs if c is not copy]

    def drain(self):
        for copy in self.recvs:
            copy.wait_recv()
        for copy in self.sends:
            copy.wait_send()


def filter_kernel(
    chunks, n_slab, n_lev, width,
    cell_hbm, value_hbm, var_hbm, frac_hbm, level_hbm, ens_hbm, loc_hbm,
    ens, loc_last, dev_out, gain_out, level_out, mean_out,
    loc_first, cell_ref, value_ref, var_ref, frac_ref, level_ref, abuf, bbuf, acc, level_wide,
    small_sem, ens_sem, own_sem, a_send, a_recv, b_send, b_recv, l_send, l_recv,
):
    slab = lax.axis_index("slab")
    lev = lax.axis_index("lev")
    lev_rows, members, cols = ens.shape
    n_obs = cell_ref.shape[1]
    loc = (loc_first, loc_last)
    total_cols = cols * n_slab
    half = members // 2
    remote = Tracker()

    barrier = pltpu.get_barrier_semaphore()
    slab_peer = [lax.rem(slab + k, n_slab) for k in range(n_slab)]
    lev_peer = [lax.rem(lev + k, n_lev) for k in range(n_lev)]
    for k in range(1, n_slab):
        pl.semaphore_signal(barrier, inc=1, device_id=(slab_peer[k], lev), device_id_type=MESH)
    for k in range(1, n_lev):
        pl.semaphore_signal(barrier, inc=1, device_id=(slab, lev_peer[k]), device_id_type=MESH)
    small_copies = [
        pltpu.make_async_copy(source, target, small_sem.at[i])
        for i, (source, target) in enumerate([
            (cell_hbm, cell_ref), (value_hbm, value_ref), (var_hbm, var_ref),
            (frac_hbm, frac_ref), (level_hbm, level_ref),
        ])
    ]
    for copy in small_copies:
        copy.start()
    ens_copies = [
        pltpu.make_async_copy(ens_hbm.at[:, l, :], ens.at[l], ens_sem.at[l])
        for l in range(lev_rows)
    ]
    for copy in ens_copies:
        copy.start()
    own_copies = [
        pltpu.make_async_copy(loc_hbm.at[b], loc[b].at[lev], own_sem.at[b]) for b in range(2)
    ]
    for copy in own_copies:
        copy.start()

    for copy in small_copies:
        copy.wait()

    slab_f = slab.astype(F32)
    lev_f = lev.astype(F32)
    rows = []
    for b in range(2):
        cell = cell_ref[pl.ds(b, 1), :].astype(F32)
        level = count_at_least(cell, total_cols, n_lev * lev_rows)
        column = cell - level * float(total_cols)
        later = column + 1.0
        later = jnp.where(later >= float(total_cols), 0.0, later)
        band = count_at_least(level, lev_rows, n_lev)
        inner = level - band * float(lev_rows)
        places = []
        for where_at in (column, later):
            in_slab = count_at_least(where_at, cols, n_slab)
            place = where_at - in_slab * float(cols) + 1.0
            places.append(jnp.where(in_slab == slab_f, place, 0.0))
        rows.append(
            [band, places[0], places[1], inner,
             value_ref[pl.ds(b, 1), :], var_ref[pl.ds(b, 1), :], frac_ref[pl.ds(b, 1), :]]
            + [level_ref[b, pl.ds(l, 1), :] for l in range(lev_rows)]
        )
    per_block = len(rows[0])
    flat = rows[0] + rows[1]
    table = jnp.concatenate(flat + [jnp.zeros((128 - len(flat), n_obs), F32)], axis=0).T

    def column_of(b, i):
        return table[:, per_block * b + i : per_block * b + i + 1]

    lane = lax.broadcasted_iota(jnp.int32, (n_obs, 128), 1)
    lane_slot = jnp.where(lane < SLOTS, lane, lane - SLOTS).astype(F32)
    first_half = lane < SLOTS
    ranks = []
    slot_info = []
    for b in range(2):
        other = lax.broadcasted_iota(jnp.int32, (n_obs, n_obs), 1)
        mine = lax.broadcasted_iota(jnp.int32, (n_obs, n_obs), 0)
        earlier = (column_of(b, 0) == rows[b][0]) & (other < mine)
        rank = jnp.sum(jnp.where(earlier, 1.0, 0.0), axis=1, keepdims=True)
        ranks.append(rank)
        per_chunk = []
        for q in range(chunks):
            chosen = (column_of(b, 0) == lev_f) & (rank == lane_slot + float(SLOTS * q))

            def picked(x):
                return jnp.sum(jnp.where(chosen, x, 0.0), axis=0, keepdims=True)

            filled = picked(jnp.ones((n_obs, 128), F32))
            place = picked(jnp.where(first_half, column_of(b, 1), column_of(b, 2))) - 1.0
            inner = picked(jnp.broadcast_to(column_of(b, 3), (n_obs, 128)))
            value = picked(jnp.broadcast_to(column_of(b, 4), (n_obs, 128)))
            var = picked(jnp.broadcast_to(column_of(b, 5), (n_obs, 128))) + (1.0 - filled)
            frac = column_of(b, 6)
            weight = picked(jnp.where(first_half, 1.0 - frac, frac))
            per_chunk.append((place, inner, value, var, weight))
        slot_info.append(per_chunk)

    def loc_copy(b, which, holder, start, count, target):
        piece = loc[b].at[holder, pl.ds(start, count)]
        return pltpu.make_async_remote_copy(
            src_ref=piece, dst_ref=piece,
            send_sem=l_send.at[b, which], recv_sem=l_recv.at[b, which],
            device_id=(slab, target), device_id_type=MESH,
        )

    up = lax.rem(lev + 2, n_lev)
    down = lax.rem(lev + n_lev - 2, n_lev)
    far = lax.rem(lev + 4, n_lev)
    mate = lev + 1 - 2 * lax.rem(lev, 2)
    held = loc_first.shape[1]
    part = held // 2
    ring = []
    for b in range(2):
        ring.append([
            loc_copy(b, 0, lev, 0, part, up),
            loc_copy(b, 1, lev, part, part, down),
            loc_copy(b, 2, lev, part, part, up),
            loc_copy(b, 3, lev, 0, part, down),
            loc_copy(b, 4, down, 0, part, up),
            loc_copy(b, 5, up, part, part, down),
            loc_copy(b, 6, lev, 0, held, mate),
            loc_copy(b, 7, down, 0, held, mate),
            loc_copy(b, 8, up, 0, held, mate),
            loc_copy(b, 9, far, 0, held, mate),
        ])

    def ring_begin(b):
        for i in (0, 1, 2, 3, 6):
            remote.start(ring[b][i])

    def ring_forward(b):
        for first, then in ((0, 4), (1, 5), (2, 7), (3, 8)):
            remote.arrived(ring[b][first])
            remote.start(ring[b][then])

    def ring_finish(b):
        remote.arrived(ring[b][4])
        remote.arrived(ring[b][5])
        remote.start(ring[b][9])
        for i in (6, 7, 8, 9):
            remote.arrived(ring[b][i])

    a_copies = [[
        pltpu.make_async_remote_copy(
            src_ref=abuf.at[r, 0], dst_ref=abuf.at[r, k],
            send_sem=a_send.at[r, k], recv_sem=a_recv.at[r, k],
            device_id=(slab_peer[k], lev), device_id_type=MESH,
        ) if k else None for k in range(n_slab)] for r in range(2)]
    b_copies = [[
        pltpu.make_async_remote_copy(
            src_ref=bbuf.at[r, 0], dst_ref=bbuf.at[r, k],
            send_sem=b_send.at[r, k], recv_sem=b_recv.at[r, k],
            device_id=(slab, lev_peer[k]), device_id_type=MESH,
        ) if k else None for k in range(n_lev)] for r in range(2)]

    lane1 = lax.broadcasted_iota(jnp.int32, (1, 128), 1)
    low1 = lane1 < SLOTS

    def send_priors(r, cells):
        for q in range(chunks):
            weighted = cells[q] * slot_info[r][q][4]
            both = weighted + pltpu.roll(weighted, SLOTS, 1)
            abuf[r, 0, q] = jnp.where(low1, both[:half], both[half:])
        for k in range(1, n_slab):
            remote.start(a_copies[r][k])

    def band_statistics(r):
        for k in range(1, n_slab):
            remote.arrived(a_copies[r][k])
        for q in range(chunks):
            packed = abuf[r, 0, q]
            for k in range(1, n_slab):
                packed = packed + abuf[r, k, q]
            turned = pltpu.roll(packed, SLOTS, 1)
            prior = jnp.concatenate(
                [jnp.where(low1, packed, turned), jnp.where(low1, turned, packed)], axis=0
            )
            _, _, value, variance, _ = slot_info[r][q]
            mean = jnp.sum(prior, axis=0, keepdims=True) / float(members)
            deviation = prior - mean
            spread = jnp.sum(deviation * deviation, axis=0, keepdims=True) / (members - 1.0)
            total = spread + variance
            shrink = 1.0 / (1.0 + jnp.sqrt(variance / total))
            gain = ((value - mean) - deviation * shrink) / (total * (members - 1.0))
            bbuf[r, 0, q, pl.ds(0, members), :] = jnp.where(low1, deviation, gain).astype(BF16)
            high, mid, low = (x.astype(F32) for x in split3(mean))
            row = lax.broadcasted_iota(jnp.int32, (16, 128), 0)
            parts = jnp.where(row == 0, high, jnp.where(row == 1, mid, jnp.where(row == 2, low, 0.0)))
            bbuf[r, 0, q, pl.ds(members, 16), :] = parts.astype(BF16)
        for k in range(1, n_lev):
            remote.start(b_copies[r][k])

    def obs_order(r):
        away = lev_f - column_of(r, 0)
        away = jnp.where(away < 0.0, away + float(n_lev), away)
        to_dev = []
        to_gain = []
        for k in range(n_lev):
            for q in range(chunks):
                chosen = (away == float(k)) & (ranks[r] == lane_slot + float(SLOTS * q))
                to_dev.append(jnp.where(chosen & first_half, 1.0, 0.0).astype(BF16))
                to_gain.append(jnp.where(chosen & ~first_half, 1.0, 0.0).astype(BF16))
        return jnp.concatenate(to_dev, axis=1), jnp.concatenate(to_gain, axis=1)

    def all_statistics(r, to_dev, to_gain):
        for k in range(1, n_lev):
            remote.arrived(b_copies[r][k])
        packed = jnp.concatenate(
            [bbuf[r, k, q] for k in range(n_lev) for q in range(chunks)], axis=1
        )
        dev = nt_dot(to_dev, packed)[:, :members].astype(BF16)
        gain = nt_dot(packed[:members], to_gain).astype(BF16)
        return dev, gain

    def all_means(r, to_dev):
        packed = jnp.concatenate(
            [bbuf[r, k, q, pl.ds(members, 16), :] for k in range(n_lev) for q in range(chunks)], axis=1
        )
        means = nt_dot(packed, to_dev)
        mean_out[pl.ds(r, 1), :] = means[0:1] + means[1:2] + means[2:3]

    def at(c):
        return pl.ds(pl.multiple_of(c * width, width), width)

    def regress(dev, gain):
        def step(c, carry):
            local = loc_first[:, :, at(c)].reshape(n_obs, width).astype(F32)
            for l in range(lev_rows):
                now = ens[l, :, at(c)]
                mean = jnp.sum(now, axis=0, keepdims=True) / float(members)
                centred = (now - mean).astype(BF16)
                cross = jnp.dot(dev, centred, preferred_element_type=F32)
                weight = jnp.tile(level_wide[l], (1, width // 128)) * local
                mixed = (weight * cross).astype(BF16)
                ens[l, :, at(c)] = now + jnp.dot(gain, mixed, preferred_element_type=F32)
            return carry

        lax.fori_loop(0, cols // width, step, 0)

    wide = 256 * chunks
    places = jnp.concatenate(
        [slot_info[b][q][0] for b in range(2) for q in range(chunks)], axis=1
    )
    inners = jnp.concatenate(
        [slot_info[b][q][1] for b in range(2) for q in range(chunks)], axis=1
    )
    at_level = [jnp.where(inners == float(l), places, -1.0) for l in range(lev_rows)]
    acc[...] = jnp.zeros_like(acc)
    for copy in ens_copies:
        copy.wait()

    step_cols = 256

    def gather_step(c, carry):
        base = c * step_cols
        here = pl.ds(pl.multiple_of(base, step_cols), step_cols)
        index = (lax.broadcasted_iota(jnp.int32, (step_cols, wide), 0) + base).astype(F32)
        hot = jnp.concatenate(
            [jnp.where(index == at_level[l], 1.0, 0.0).astype(BF16) for l in range(lev_rows)],
            axis=0,
        )
        pieces = [split3(ens[l, :, here]) for l in range(lev_rows)]
        left = jnp.concatenate(
            [jnp.concatenate([pieces[l][i] for l in range(lev_rows)], axis=1) for i in range(3)],
            axis=0,
        )
        acc[...] += jnp.dot(left, hot, preferred_element_type=F32)
        return carry

    lax.fori_loop(0, cols // step_cols, gather_step, 0)
    picked_cells = acc[:members] + acc[members : 2 * members] + acc[2 * members :]
    cells = [
        [picked_cells[:, 128 * (b * chunks + q) : 128 * (b * chunks + q + 1)] for q in range(chunks)]
        for b in range(2)
    ]

    pl.semaphore_wait(barrier, n_lev + n_slab - 2)
    send_priors(0, cells[0])
    own_copies[0].wait()
    ring_begin(0)
    to_dev, to_gain = obs_order(0)
    for l in range(lev_rows):
        level_wide[l] = jnp.broadcast_to(column_of(0, 7 + l), (n_obs, 128))
    level_out[...] = table
    ring_forward(0)
    own_copies[1].wait()
    band_statistics(0)
    ring_finish(0)

    later_places = jnp.concatenate([slot_info[1][q][0] for q in range(chunks)], axis=1)
    later_inners = jnp.concatenate([slot_info[1][q][1] for q in range(chunks)], axis=1)
    narrow = 128 * chunks
    index = lax.broadcasted_iota(jnp.int32, (cols, narrow), 0).astype(F32)
    hot = jnp.where(index == later_places, 1.0, 0.0).astype(BF16)
    weights = jnp.dot(loc_first[...].reshape(n_obs, cols), hot, preferred_element_type=F32)
    level_weight = jnp.zeros((n_obs, narrow), F32)
    for l in range(lev_rows):
        level_weight = jnp.where(later_inners == float(l), column_of(0, 7 + l), level_weight)
    weights = level_weight * weights

    dev, gain = all_statistics(0, to_dev, to_gain)
    ring_begin(1)
    now = jnp.concatenate(cells[1], axis=1)
    centred = (now - jnp.sum(now, axis=0, keepdims=True) / float(members)).astype(BF16)
    cross = jnp.dot(dev, centred, preferred_element_type=F32)
    mixed = (weights * cross).astype(BF16)
    now = now + jnp.dot(gain, mixed, preferred_element_type=F32)
    send_priors(1, [now[:, 128 * q : 128 * (q + 1)] for q in range(chunks)])
    all_means(0, to_dev)
    regress(dev, gain)
    ring_forward(1)
    to_dev, to_gain = obs_order(1)
    band_statistics(1)
    ring_finish(1)
    dev, gain = all_statistics(1, to_dev, to_gain)
    dev_out[...] = dev
    gain_out[...] = gain
    all_means(1, to_dev)
    remote.drain()


def run_filter(chunks, n_slab, n_lev, obs_cell, obs_value, obs_var, obs_frac, loc_level, ensemble, loc_column):
    members, lev_rows, cols = ensemble.shape
    n_obs = obs_cell.shape[1]
    held = loc_column.shape[1]
    width = WIDTH if cols % WIDTH == 0 else cols
    vmem = pl.BlockSpec(memory_space=pltpu.VMEM)
    hbm = pl.BlockSpec(memory_space=pltpu.HBM)
    dma = pltpu.SemaphoreType.DMA
    return pl.pallas_call(
        functools.partial(filter_kernel, chunks, n_slab, n_lev, width),
        out_shape=(
            jax.ShapeDtypeStruct((lev_rows, members, cols), F32),
            jax.ShapeDtypeStruct((n_lev, held, cols), BF16),
            jax.ShapeDtypeStruct((n_obs, members), BF16),
            jax.ShapeDtypeStruct((members, n_obs), BF16),
            jax.ShapeDtypeStruct((n_obs, 128), F32),
            jax.ShapeDtypeStruct((2, n_obs), F32),
        ),
        in_specs=[hbm] * 7,
        out_specs=(vmem,) * 6,
        scratch_shapes=[
            pltpu.VMEM((n_lev, held, cols), BF16),
            pltpu.VMEM(obs_cell.shape, jnp.int32),
            pltpu.VMEM(obs_cell.shape, F32),
            pltpu.VMEM(obs_cell.shape, F32),
            pltpu.VMEM(obs_cell.shape, F32),
            pltpu.VMEM(loc_level.shape, F32),
            pltpu.VMEM((2, n_slab, chunks, members // 2, 128), F32),
            pltpu.VMEM((2, n_lev, chunks, members + 16, 128), BF16),
            pltpu.VMEM((3 * members, 256 * chunks), F32),
            pltpu.VMEM((lev_rows, n_obs, 128), F32),
            dma((5,)),
            dma((lev_rows,)),
            dma((2,)),
            dma((2, n_slab)),
            dma((2, n_slab)),
            dma((2, n_lev)),
            dma((2, n_lev)),
            dma((2, 10)),
            dma((2, 10)),
        ],
        compiler_params=pltpu.CompilerParams(
            collective_id=chunks, has_side_effects=True, vmem_limit_bytes=VMEM_LIMIT
        ),
    )(obs_cell, obs_value, obs_var, obs_frac, loc_level, ensemble, loc_column)


def last_kernel(ens, loc, dev_ref, gain_ref, level_ref, out_hbm, out, out_sem):
    lev_rows, members, cols = ens.shape
    n_obs = dev_ref.shape[0]
    dev = dev_ref[...]
    gain = gain_ref[...]
    copies = []
    for l in range(lev_rows):
        now = ens[l]
        mean = jnp.sum(now, axis=0, keepdims=True) / float(members)
        centred = (now - mean).astype(BF16)
        cross = jnp.dot(dev, centred, preferred_element_type=F32)
        place = LEVEL_AT + l
        weight = level_ref[:, place : place + 1] * loc[...].reshape(n_obs, cols).astype(F32)
        mixed = (weight * cross).astype(BF16)
        out[l] = now + jnp.dot(gain, mixed, preferred_element_type=F32)
        copies.append(pltpu.make_async_copy(out.at[l], out_hbm.at[:, l, :], out_sem.at[l]))
        copies[l].start()
    for copy in copies:
        copy.wait()


LEVEL_AT = 18
VMEM_LIMIT = 40 * 1024 * 1024
WIDTH = 2304
COND = True


def last_update(ens, loc, dev, gain, level):
    lev_rows, members, cols = ens.shape
    vmem = pl.BlockSpec(memory_space=pltpu.VMEM)
    return pl.pallas_call(
        last_kernel,
        out_shape=pltpu.HBM((members, lev_rows, cols), F32),
        in_specs=[vmem] * 5,
        out_specs=pl.BlockSpec(memory_space=pltpu.HBM),
        scratch_shapes=[
            pltpu.VMEM((lev_rows, members, cols), F32),
            pltpu.SemaphoreType.DMA((lev_rows,)),
        ],
        compiler_params=pltpu.CompilerParams(vmem_limit_bytes=VMEM_LIMIT),
    )(ens, loc, dev, gain, level)


def on_device(n_slab, n_lev, ensemble, obs_cell, obs_value, obs_var, obs_frac, loc_column, loc_level):
    members, lev_rows, slab_cols = ensemble.shape
    n_obs = obs_cell.shape[1]
    operands = (obs_cell, obs_value, obs_var, obs_frac, jnp.swapaxes(loc_level, 1, 2), ensemble, loc_column)

    def whole(chunks, *arrays):
        state = run_filter(chunks, n_slab, n_lev, *arrays)
        return last_update(*state[:5]), state[5]

    if not COND:
        return whole(1, *operands)
    band_cells = slab_cols * n_slab * lev_rows
    starts = jnp.arange(n_lev, dtype=jnp.int32) * band_cells
    cell = obs_cell[:, :, None]
    inside = (cell >= starts) & (cell < starts + band_cells)
    crowd = jnp.max(jnp.sum(inside.astype(jnp.int32), axis=1))
    return lax.cond(
        crowd <= SLOTS, functools.partial(whole, 1), functools.partial(whole, 3), *operands
    )


def solution(mesh):
    in_specs = (
        P(None, "lev", "slab"),
        P(),
        P(),
        P(),
        P(),
        P(None, "lev", "slab"),
        P(None, None, "lev"),
    )
    out_specs = (P(None, "lev", "slab"), P())
    return jax.shard_map(
        functools.partial(on_device, mesh.shape["slab"], mesh.shape["lev"]),
        mesh=mesh, in_specs=in_specs, out_specs=out_specs, check_vma=False,
    )
```

```python
import functools

import jax
import jax.numpy as jnp
from jax import lax
from jax.experimental import pallas as pl
from jax.experimental.pallas import tpu as pltpu
from jax.sharding import PartitionSpec as P

MESH = pl.DeviceIdType.MESH
SLOTS = 64
F32 = jnp.float32
BF16 = jnp.bfloat16


def nt_dot(a, b):
    return lax.dot_general(a, b, (((1,), (1,)), ((), ())), preferred_element_type=F32)


def count_at_least(x, step, number):
    total = jnp.zeros_like(x)
    for k in range(1, number):
        total = total + jnp.where(x >= float(k * step), 1.0, 0.0)
    return total


def split3(x):
    high = x.astype(BF16)
    rest = x - high.astype(F32)
    mid = rest.astype(BF16)
    low = (rest - mid.astype(F32)).astype(BF16)
    return high, mid, low


class Tracker:
    def __init__(self):
        self.sends = []
        self.recvs = []

    def start(self, copy):
        copy.start()
        self.sends.append(copy)
        self.recvs.append(copy)

    def arrived(self, copy):
        copy.wait_recv()
        self.recvs = [c for c in self.recvs if c is not copy]

    def drain(self):
        for copy in self.recvs:
            copy.wait_recv()
        for copy in self.sends:
            copy.wait_send()


def filter_kernel(
    chunks, n_slab, n_lev, width,
    cell_hbm, value_hbm, var_hbm, frac_hbm, level_hbm, ens_hbm, loc_hbm,
    ens, loc_last, dev_out, gain_out, level_out, mean_out, crowd_out,
    loc_first, cell_ref, value_ref, var_ref, frac_ref, level_ref, abuf, bbuf, level_wide,
    small_sem, ens_sem, own_sem, a_send, a_recv, b_send, b_recv, l_send, l_recv,
):
    slab = lax.axis_index("slab")
    lev = lax.axis_index("lev")
    lev_rows, members, cols = ens.shape
    n_obs = cell_ref.shape[1]
    loc = (loc_first, loc_last)
    total_cols = cols * n_slab
    half = members // 2
    remote = Tracker()

    barrier = pltpu.get_barrier_semaphore()
    slab_peer = [lax.rem(slab + k, n_slab) for k in range(n_slab)]
    lev_peer = [lax.rem(lev + k, n_lev) for k in range(n_lev)]
    for k in range(1, n_slab):
        pl.semaphore_signal(barrier, inc=1, device_id=(slab_peer[k], lev), device_id_type=MESH)
    for k in range(1, n_lev):
        pl.semaphore_signal(barrier, inc=1, device_id=(slab, lev_peer[k]), device_id_type=MESH)
    small_copies = [
        pltpu.make_async_copy(source, target, small_sem.at[i])
        for i, (source, target) in enumerate([
            (cell_hbm, cell_ref), (value_hbm, value_ref), (var_hbm, var_ref),
            (frac_hbm, frac_ref), (level_hbm, level_ref),
        ])
    ]
    for copy in small_copies:
        copy.start()
    ens_copies = [
        pltpu.make_async_copy(ens_hbm.at[:, l, :], ens.at[l], ens_sem.at[l])
        for l in range(lev_rows)
    ]
    for copy in ens_copies:
        copy.start()
    own_copies = [
        pltpu.make_async_copy(loc_hbm.at[b], loc[b].at[lev], own_sem.at[b]) for b in range(2)
    ]
    for copy in own_copies:
        copy.start()

    for copy in small_copies:
        copy.wait()

    slab_f = slab.astype(F32)
    lev_f = lev.astype(F32)
    lane = lax.broadcasted_iota(jnp.int32, (n_obs, 128), 1)
    lane_slot = jnp.where(lane < SLOTS, lane, lane - SLOTS).astype(F32)
    first_half = lane < SLOTS

    def locate(b):
        cell = cell_ref[pl.ds(b, 1), :].astype(F32)
        level = count_at_least(cell, total_cols, n_lev * lev_rows)
        column = cell - level * float(total_cols)
        later = column + 1.0
        later = jnp.where(later >= float(total_cols), 0.0, later)
        band = count_at_least(level, lev_rows, n_lev)
        inner = level - band * float(lev_rows)
        places = []
        for where_at in (column, later):
            in_slab = count_at_least(where_at, cols, n_slab)
            place = where_at - in_slab * float(cols) + 1.0
            places.append(jnp.where(in_slab == slab_f, place, 0.0))
        flat = [band, places[0], places[1], inner,
                value_ref[pl.ds(b, 1), :], var_ref[pl.ds(b, 1), :], frac_ref[pl.ds(b, 1), :]]
        flat = flat + [level_ref[b, pl.ds(l, 1), :] for l in range(lev_rows)]
        table = jnp.concatenate(flat + [jnp.zeros((128 - len(flat), n_obs), F32)], axis=0).T
        other = lax.broadcasted_iota(jnp.int32, (n_obs, n_obs), 1)
        mine = lax.broadcasted_iota(jnp.int32, (n_obs, n_obs), 0)
        earlier = (table[:, 0:1] == band) & (other < mine)
        rank = jnp.sum(jnp.where(earlier, 1.0, 0.0), axis=1, keepdims=True)
        return table, rank, jnp.max(rank)

    def column_of(found, i):
        return found[0][:, i : i + 1]

    def picked(found, q, x):
        chosen = (column_of(found, 0) == lev_f) & (found[1] == lane_slot + float(SLOTS * q))
        return jnp.sum(jnp.where(chosen, x, 0.0), axis=0, keepdims=True)

    def slot_places(found):
        place = jnp.where(first_half, column_of(found, 1), column_of(found, 2))
        inner = jnp.broadcast_to(column_of(found, 3), (n_obs, 128))
        return (
            jnp.concatenate([picked(found, q, place) - 1.0 for q in range(chunks)], axis=1),
            jnp.concatenate([picked(found, q, inner) for q in range(chunks)], axis=1),
        )

    def slot_weights(found):
        frac = column_of(found, 6)
        weight = jnp.where(first_half, 1.0 - frac, frac)
        return [picked(found, q, weight) for q in range(chunks)]

    def slot_values(found):
        pairs = []
        for q in range(chunks):
            value = picked(found, q, column_of(found, 4))
            var = picked(found, q, column_of(found, 5) - 1.0) + 1.0
            pairs.append((value, var))
        return pairs

    def gather_cells(places, inners):
        index = lax.broadcasted_iota(jnp.int32, (cols, 128 * chunks), 0).astype(F32)
        hot = jnp.where(index == places, 1.0, 0.0).astype(BF16)
        cells = jnp.zeros((members, 128 * chunks), F32)
        for l in range(lev_rows):
            left = jnp.concatenate(split3(ens[l])[:PIECES], axis=0)
            found = jnp.dot(left, hot, preferred_element_type=F32)
            total = found[:members]
            for i in range(1, PIECES):
                total = total + found[i * members : (i + 1) * members]
            cells = jnp.where(inners == float(l), total, cells)
        return hot, jnp.where(places >= 0.0, cells, 0.0)

    def loc_copy(b, which, holder, start, count, target):
        piece = loc[b].at[holder, pl.ds(start, count)]
        return pltpu.make_async_remote_copy(
            src_ref=piece, dst_ref=piece,
            send_sem=l_send.at[b, which], recv_sem=l_recv.at[b, which],
            device_id=(slab, target), device_id_type=MESH,
        )

    up = lax.rem(lev + 2, n_lev)
    down = lax.rem(lev + n_lev - 2, n_lev)
    far = lax.rem(lev + 4, n_lev)
    mate = lev + 1 - 2 * lax.rem(lev, 2)
    held = loc_first.shape[1]
    part = held // 2
    ring = []
    for b in range(2):
        ring.append([
            loc_copy(b, 0, lev, 0, part, up),
            loc_copy(b, 1, lev, part, part, down),
            loc_copy(b, 2, lev, part, part, up),
            loc_copy(b, 3, lev, 0, part, down),
            loc_copy(b, 4, down, 0, part, up),
            loc_copy(b, 5, up, part, part, down),
            loc_copy(b, 6, lev, 0, held, mate),
            loc_copy(b, 7, down, 0, held, mate),
            loc_copy(b, 8, up, 0, held, mate),
            loc_copy(b, 9, far, 0, held, mate),
        ])

    def ring_begin(b):
        for i in (0, 1, 2, 3, 6):
            remote.start(ring[b][i])

    def ring_forward(b):
        for first, then in ((0, 4), (1, 5), (2, 7), (3, 8)):
            remote.arrived(ring[b][first])
            remote.start(ring[b][then])

    def ring_finish(b):
        remote.arrived(ring[b][4])
        remote.arrived(ring[b][5])
        remote.start(ring[b][9])
        for i in (6, 7, 8, 9):
            remote.arrived(ring[b][i])

    a_copies = [[
        pltpu.make_async_remote_copy(
            src_ref=abuf.at[r, 0], dst_ref=abuf.at[r, k],
            send_sem=a_send.at[r, k], recv_sem=a_recv.at[r, k],
            device_id=(slab_peer[k], lev), device_id_type=MESH,
        ) if k else None for k in range(n_slab)] for r in range(2)]
    b_copies = [[
        pltpu.make_async_remote_copy(
            src_ref=bbuf.at[r, 0], dst_ref=bbuf.at[r, k],
            send_sem=b_send.at[r, k], recv_sem=b_recv.at[r, k],
            device_id=(slab, lev_peer[k]), device_id_type=MESH,
        ) if k else None for k in range(n_lev)] for r in range(2)]

    lane1 = lax.broadcasted_iota(jnp.int32, (1, 128), 1)
    low1 = lane1 < SLOTS

    def send_priors(r, cells, weights):
        for q in range(chunks):
            weighted = cells[:, 128 * q : 128 * (q + 1)] * weights[q]
            both = weighted + pltpu.roll(weighted, SLOTS, 1)
            abuf[r, 0, q] = jnp.where(low1, both[:half], both[half:])
        for k in range(1, n_slab):
            remote.start(a_copies[r][k])

    def band_statistics(r, values):
        for k in range(1, n_slab):
            remote.arrived(a_copies[r][k])
        for q in range(chunks):
            packed = abuf[r, 0, q]
            for k in range(1, n_slab):
                packed = packed + abuf[r, k, q]
            turned = pltpu.roll(packed, SLOTS, 1)
            prior = jnp.concatenate(
                [jnp.where(low1, packed, turned), jnp.where(low1, turned, packed)], axis=0
            )
            value, variance = values[q]
            mean = jnp.sum(prior, axis=0, keepdims=True) / float(members)
            deviation = prior - mean
            spread = jnp.sum(deviation * deviation, axis=0, keepdims=True) / (members - 1.0)
            total = spread + variance
            shrink = 1.0 / (1.0 + jnp.sqrt(variance / total))
            gain = ((value - mean) - deviation * shrink) / (total * (members - 1.0))
            bbuf[r, 0, q, pl.ds(0, members), :] = jnp.where(low1, deviation, gain).astype(BF16)
            high, mid, low = (x.astype(F32) for x in split3(mean))
            row = lax.broadcasted_iota(jnp.int32, (16, 128), 0)
            parts = jnp.where(row == 0, high, jnp.where(row == 1, mid, jnp.where(row == 2, low, 0.0)))
            bbuf[r, 0, q, pl.ds(members, 16), :] = parts.astype(BF16)
        for k in range(1, n_lev):
            remote.start(b_copies[r][k])

    def obs_order(found):
        away = lev_f - column_of(found, 0)
        away = jnp.where(away < 0.0, away + float(n_lev), away)
        to_dev = []
        to_gain = []
        for k in range(n_lev):
            for q in range(chunks):
                chosen = (away == float(k)) & (found[1] == lane_slot + float(SLOTS * q))
                to_dev.append(jnp.where(chosen & first_half, 1.0, 0.0).astype(BF16))
                to_gain.append(jnp.where(chosen & ~first_half, 1.0, 0.0).astype(BF16))
        return jnp.concatenate(to_dev, axis=1), jnp.concatenate(to_gain, axis=1)

    def all_statistics(r, to_dev, to_gain):
        for k in range(1, n_lev):
            remote.arrived(b_copies[r][k])
        packed = jnp.concatenate(
            [bbuf[r, k, q] for k in range(n_lev) for q in range(chunks)], axis=1
        )
        dev = nt_dot(to_dev, packed)[:, :members].astype(BF16)
        gain = nt_dot(packed[:members], to_gain).astype(BF16)
        return dev, gain

    def all_means(r, to_dev):
        packed = jnp.concatenate(
            [bbuf[r, k, q, pl.ds(members, 16), :] for k in range(n_lev) for q in range(chunks)], axis=1
        )
        means = nt_dot(packed, to_dev)
        mean_out[pl.ds(r, 1), :] = means[0:1] + means[1:2] + means[2:3]

    def at(c):
        return pl.ds(pl.multiple_of(c * width, width), width)

    def regress(dev, gain):
        def step(c, carry):
            local = loc_first[:, :, at(c)].reshape(n_obs, width).astype(F32)
            for l in range(lev_rows):
                now = ens[l, :, at(c)]
                mean = jnp.sum(now, axis=0, keepdims=True) / float(members)
                centred = (now - mean).astype(BF16)
                cross = jnp.dot(dev, centred, preferred_element_type=F32)
                weight = jnp.tile(level_wide[l], (1, width // 128)) * local
                mixed = (weight * cross).astype(BF16)
                ens[l, :, at(c)] = now + jnp.dot(gain, mixed, preferred_element_type=F32)
            return carry

        lax.fori_loop(0, cols // width, step, 0)

    found0 = locate(0)
    places, inners = slot_places(found0)
    weights0 = slot_weights(found0)
    for copy in ens_copies:
        copy.wait()
    _, cells = gather_cells(places, inners)
    pl.semaphore_wait(barrier, n_lev + n_slab - 2)
    send_priors(0, cells, weights0)
    own_copies[0].wait()
    ring_begin(0)

    values0 = slot_values(found0)
    found1 = locate(1)
    places, inners = slot_places(found1)
    weights1 = slot_weights(found1)
    hot, now = gather_cells(places, inners)
    to_dev, to_gain = obs_order(found0)
    ring_forward(0)
    own_copies[1].wait()
    band_statistics(0, values0)
    for l in range(lev_rows):
        level_wide[l] = jnp.broadcast_to(column_of(found0, 7 + l), (n_obs, 128))
    level_out[...] = found1[0]
    ring_finish(0)

    weights = jnp.dot(loc_first[...].reshape(n_obs, cols), hot, preferred_element_type=F32)
    level_weight = jnp.zeros((n_obs, 128 * chunks), F32)
    for l in range(lev_rows):
        level_weight = jnp.where(inners == float(l), column_of(found0, 7 + l), level_weight)
    weights = level_weight * weights
    centred = (now - jnp.sum(now, axis=0, keepdims=True) / float(members)).astype(BF16)

    dev, gain = all_statistics(0, to_dev, to_gain)
    cross = jnp.dot(dev, centred, preferred_element_type=F32)
    mixed = (weights * cross).astype(BF16)
    now = now + jnp.dot(gain, mixed, preferred_element_type=F32)
    send_priors(1, now, weights1)
    ring_begin(1)

    crowd_out[0] = (jnp.maximum(found0[2], found1[2]) >= float(SLOTS * chunks)).astype(jnp.int32)
    all_means(0, to_dev)
    values1 = slot_values(found1)
    regress(dev, gain)
    to_dev, to_gain = obs_order(found1)
    ring_forward(1)
    band_statistics(1, values1)
    ring_finish(1)
    dev, gain = all_statistics(1, to_dev, to_gain)
    dev_out[...] = dev
    gain_out[...] = gain
    all_means(1, to_dev)
    remote.drain()


def run_filter(chunks, n_slab, n_lev, obs_cell, obs_value, obs_var, obs_frac, loc_level, ensemble, loc_column):
    members, lev_rows, cols = ensemble.shape
    n_obs = obs_cell.shape[1]
    held = loc_column.shape[1]
    width = WIDTH if cols % WIDTH == 0 else cols
    vmem = pl.BlockSpec(memory_space=pltpu.VMEM)
    hbm = pl.BlockSpec(memory_space=pltpu.HBM)
    dma = pltpu.SemaphoreType.DMA
    return pl.pallas_call(
        functools.partial(filter_kernel, chunks, n_slab, n_lev, width),
        out_shape=(
            pltpu.VMEM((lev_rows, members, cols), F32),
            pltpu.VMEM((n_lev, held, cols), BF16),
            pltpu.VMEM((n_obs, members), BF16),
            pltpu.VMEM((members, n_obs), BF16),
            pltpu.VMEM((n_obs, 128), F32),
            pltpu.VMEM((2, n_obs), F32),
            jax.ShapeDtypeStruct((1,), jnp.int32),
        ),
        in_specs=[hbm] * 7,
        out_specs=(vmem,) * 6 + (pl.BlockSpec(memory_space=pltpu.SMEM),),
        scratch_shapes=[
            pltpu.VMEM((n_lev, held, cols), BF16),
            pltpu.VMEM(obs_cell.shape, jnp.int32),
            pltpu.VMEM(obs_cell.shape, F32),
            pltpu.VMEM(obs_cell.shape, F32),
            pltpu.VMEM(obs_cell.shape, F32),
            pltpu.VMEM(loc_level.shape, F32),
            pltpu.VMEM((2, n_slab, chunks, members // 2, 128), F32),
            pltpu.VMEM((2, n_lev, chunks, members + 16, 128), BF16),
            pltpu.VMEM((lev_rows, n_obs, 128), F32),
            dma((5,)),
            dma((lev_rows,)),
            dma((2,)),
            dma((2, n_slab)),
            dma((2, n_slab)),
            dma((2, n_lev)),
            dma((2, n_lev)),
            dma((2, 10)),
            dma((2, 10)),
        ],
        compiler_params=pltpu.CompilerParams(
            collective_id=chunks, has_side_effects=True, vmem_limit_bytes=VMEM_LIMIT
        ),
    )(*(pltpu.with_memory_space_constraint(x, pltpu.HBM) for x in (
        obs_cell, obs_value, obs_var, obs_frac, loc_level, ensemble, loc_column)))


def last_kernel(ens, loc, dev_ref, gain_ref, level_ref, mean_ref, out_hbm, mean_hbm, out, out_sem, mean_sem):
    lev_rows, members, cols = ens.shape
    n_obs = dev_ref.shape[0]
    dev = dev_ref[...]
    gain = gain_ref[...]
    copies = [pltpu.make_async_copy(mean_ref, mean_hbm, mean_sem)]
    copies[0].start()
    for l in range(lev_rows):
        now = ens[l]
        mean = jnp.sum(now, axis=0, keepdims=True) / float(members)
        centred = (now - mean).astype(BF16)
        cross = jnp.dot(dev, centred, preferred_element_type=F32)
        place = LEVEL_AT + l
        weight = level_ref[:, place : place + 1] * loc[...].reshape(n_obs, cols).astype(F32)
        mixed = (weight * cross).astype(BF16)
        out[l] = now + jnp.dot(gain, mixed, preferred_element_type=F32)
        copies.append(pltpu.make_async_copy(out.at[l], out_hbm.at[:, l, :], out_sem.at[l]))
        copies[l + 1].start()
    for copy in copies:
        copy.wait()


LEVEL_AT = 7
PIECES = 3
VMEM_LIMIT = 40 * 1024 * 1024
WIDTH = 2304
COND = True


def last_update(ens, loc, dev, gain, level, mean):
    lev_rows, members, cols = ens.shape
    vmem = pl.BlockSpec(memory_space=pltpu.VMEM)
    hbm = pl.BlockSpec(memory_space=pltpu.HBM)
    return pl.pallas_call(
        last_kernel,
        out_shape=(pltpu.HBM((members, lev_rows, cols), F32), pltpu.HBM(mean.shape, F32)),
        in_specs=[vmem] * 6,
        out_specs=(hbm, hbm),
        scratch_shapes=[
            pltpu.VMEM((lev_rows, members, cols), F32),
            pltpu.SemaphoreType.DMA((lev_rows,)),
            pltpu.SemaphoreType.DMA,
        ],
        compiler_params=pltpu.CompilerParams(vmem_limit_bytes=VMEM_LIMIT),
    )(*(pltpu.with_memory_space_constraint(x, pltpu.VMEM) for x in (ens, loc, dev, gain, level, mean)))


def on_device(n_slab, n_lev, ensemble, obs_cell, obs_value, obs_var, obs_frac, loc_column, loc_level):
    members, lev_rows, slab_cols = ensemble.shape
    n_obs = obs_cell.shape[1]
    operands = (obs_cell, obs_value, obs_var, obs_frac, jnp.swapaxes(loc_level, 1, 2), ensemble, loc_column)

    def whole(chunks):
        *state, crowd = run_filter(chunks, n_slab, n_lev, *operands)
        return (crowd[0], *last_update(*state))

    done = lax.while_loop(lambda state: state[0] != 0, lambda state: whole(3), whole(1))
    return done[1], done[2]


def solution(mesh):
    in_specs = (
        P(None, "lev", "slab"),
        P(),
        P(),
        P(),
        P(),
        P(None, "lev", "slab"),
        P(None, None, "lev"),
    )
    out_specs = (P(None, "lev", "slab"), P())
    return jax.shard_map(
        functools.partial(on_device, mesh.shape["slab"], mesh.shape["lev"]),
        mesh=mesh, in_specs=in_specs, out_specs=out_specs, check_vma=False,
    )
```

```python
import functools
import math

import jax
import jax.numpy as jnp
from jax import lax
from jax.experimental import pallas as pl
from jax.experimental.pallas import tpu as pltpu
from jax.sharding import PartitionSpec as P

MESH = pl.DeviceIdType.MESH
SLOTS = 64
F32 = jnp.float32
BF16 = jnp.bfloat16


def nt_dot(a, b):
    return lax.dot_general(a, b, (((1,), (1,)), ((), ())), preferred_element_type=F32)


def count_at_least(x, step, number):
    total = jnp.zeros_like(x)
    for k in range(1, number):
        total = total + jnp.where(x >= float(k * step), 1.0, 0.0)
    return total


def split3(x):
    high = x.astype(BF16)
    rest = x - high.astype(F32)
    mid = rest.astype(BF16)
    low = (rest - mid.astype(F32)).astype(BF16)
    return high, mid, low


class Tracker:
    def __init__(self):
        self.sends = []
        self.recvs = []

    def start(self, copy):
        copy.start()
        self.sends.append(copy)
        self.recvs.append(copy)

    def arrived(self, copy):
        copy.wait_recv()
        self.recvs = [c for c in self.recvs if c is not copy]

    def drain(self):
        for copy in self.recvs:
            copy.wait_recv()
        for copy in self.sends:
            copy.wait_send()


def filter_kernel(
    chunks, n_slab, n_lev, width,
    cell_hbm, value_hbm, var_hbm, frac_hbm, level_hbm, ens_hbm, loc_hbm,
    ens, loc_last, dev_out, gain_out, level_out, mean_out, crowd_out,
    loc_first, cell_ref, value_ref, var_ref, frac_ref, level_ref, abuf, bbuf, level_wide,
    small_sem, ens_sem, own_sem, a_send, a_recv, b_send, b_recv, l_send, l_recv,
):
    slab = lax.axis_index("slab")
    lev = lax.axis_index("lev")
    lev_rows, members, cols = ens.shape
    n_obs = cell_ref.shape[1]
    loc = (loc_first, loc_last)
    total_cols = cols * n_slab
    half = members // 2
    remote = Tracker()

    barrier = pltpu.get_barrier_semaphore()
    side = math.isqrt(n_slab)
    stack = n_lev // 2

    def around(k, n):
        return min(k, n - k)

    slab_peer = [
        lax.rem(slab // side + k // side, side) * side + lax.rem(lax.rem(slab, side) + k % side, side)
        for k in range(n_slab)
    ]
    core = lax.rem(lev, 2)
    lev_peer = [
        lax.rem(lev // 2 + k // 2, stack) * 2 + (1 - core if k % 2 else core) for k in range(n_lev)
    ]
    slab_order = sorted(
        range(1, n_slab), key=lambda k: -around(k // side, side) - around(k % side, side)
    )
    lev_order = sorted(range(1, n_lev), key=lambda k: -around(k // 2, stack))
    for k in slab_order:
        pl.semaphore_signal(barrier, inc=1, device_id=(slab_peer[k], lev), device_id_type=MESH)
    for k in lev_order:
        pl.semaphore_signal(barrier, inc=1, device_id=(slab, lev_peer[k]), device_id_type=MESH)
    small_copies = [
        pltpu.make_async_copy(source, target, small_sem.at[i])
        for i, (source, target) in enumerate([
            (cell_hbm, cell_ref), (value_hbm, value_ref), (var_hbm, var_ref),
            (frac_hbm, frac_ref), (level_hbm, level_ref),
        ])
    ]
    for copy in small_copies:
        copy.start()
    ens_copies = [
        pltpu.make_async_copy(ens_hbm.at[:, l, :], ens.at[l], ens_sem.at[l])
        for l in range(lev_rows)
    ]
    for copy in ens_copies:
        copy.start()
    own_copies = [
        pltpu.make_async_copy(loc_hbm.at[b], loc[b].at[lev], own_sem.at[b]) for b in range(2)
    ]
    for copy in own_copies:
        copy.start()

    for copy in small_copies:
        copy.wait()

    slab_f = slab.astype(F32)
    lev_f = lev.astype(F32)
    lane = lax.broadcasted_iota(jnp.int32, (n_obs, 128), 1)
    lane_slot = jnp.where(lane < SLOTS, lane, lane - SLOTS).astype(F32)
    first_half = lane < SLOTS

    def locate(b):
        cell = cell_ref[pl.ds(b, 1), :].astype(F32)
        level = count_at_least(cell, total_cols, n_lev * lev_rows)
        column = cell - level * float(total_cols)
        later = column + 1.0
        later = jnp.where(later >= float(total_cols), 0.0, later)
        band = count_at_least(level, lev_rows, n_lev)
        inner = level - band * float(lev_rows)
        places = []
        for where_at in (column, later):
            in_slab = count_at_least(where_at, cols, n_slab)
            place = where_at - in_slab * float(cols) + 1.0
            places.append(jnp.where(in_slab == slab_f, place, 0.0))
        flat = [band, places[0], places[1], inner,
                value_ref[pl.ds(b, 1), :], var_ref[pl.ds(b, 1), :], frac_ref[pl.ds(b, 1), :]]
        flat = flat + [level_ref[b, pl.ds(l, 1), :] for l in range(lev_rows)]
        table = jnp.concatenate(flat + [jnp.zeros((128 - len(flat), n_obs), F32)], axis=0).T
        other = lax.broadcasted_iota(jnp.int32, (n_obs, n_obs), 1)
        mine = lax.broadcasted_iota(jnp.int32, (n_obs, n_obs), 0)
        earlier = (table[:, 0:1] == band) & (other < mine)
        rank = jnp.sum(jnp.where(earlier, 1.0, 0.0), axis=1, keepdims=True)
        return table, rank, jnp.max(rank)

    def column_of(found, i):
        return found[0][:, i : i + 1]

    def picked(found, q, x):
        chosen = (column_of(found, 0) == lev_f) & (found[1] == lane_slot + float(SLOTS * q))
        return jnp.sum(jnp.where(chosen, x, 0.0), axis=0, keepdims=True)

    def slot_places(found):
        place = jnp.where(first_half, column_of(found, 1), column_of(found, 2))
        inner = jnp.broadcast_to(column_of(found, 3), (n_obs, 128))
        return (
            jnp.concatenate([picked(found, q, place) - 1.0 for q in range(chunks)], axis=1),
            jnp.concatenate([picked(found, q, inner) for q in range(chunks)], axis=1),
        )

    def slot_weights(found):
        frac = column_of(found, 6)
        weight = jnp.where(first_half, 1.0 - frac, frac)
        return [picked(found, q, weight) for q in range(chunks)]

    def slot_values(found):
        pairs = []
        for q in range(chunks):
            value = picked(found, q, column_of(found, 4))
            var = picked(found, q, column_of(found, 5) - 1.0) + 1.0
            pairs.append((value, var))
        return pairs

    def gather_cells(places, inners):
        index = lax.broadcasted_iota(jnp.int32, (cols, 128 * chunks), 0).astype(F32)
        hot = jnp.where(index == places, 1.0, 0.0).astype(BF16)
        cells = jnp.zeros((members, 128 * chunks), F32)
        for l in range(lev_rows):
            left = jnp.concatenate(split3(ens[l])[:PIECES], axis=0)
            found = jnp.dot(left, hot, preferred_element_type=F32)
            total = found[:members]
            for i in range(1, PIECES):
                total = total + found[i * members : (i + 1) * members]
            cells = jnp.where(inners == float(l), total, cells)
        return hot, jnp.where(places >= 0.0, cells, 0.0)

    def loc_copy(b, which, holder, start, count, target):
        piece = loc[b].at[holder, pl.ds(start, count)]
        return pltpu.make_async_remote_copy(
            src_ref=piece, dst_ref=piece,
            send_sem=l_send.at[b, which], recv_sem=l_recv.at[b, which],
            device_id=(slab, target), device_id_type=MESH,
        )

    up = lax.rem(lev + 2, n_lev)
    down = lax.rem(lev + n_lev - 2, n_lev)
    far = lax.rem(lev + 4, n_lev)
    mate = lev + 1 - 2 * lax.rem(lev, 2)
    held = loc_first.shape[1]
    part = held // 2
    ring = []
    for b in range(2):
        ring.append([
            loc_copy(b, 0, lev, 0, part, up),
            loc_copy(b, 1, lev, part, part, down),
            loc_copy(b, 2, lev, part, part, up),
            loc_copy(b, 3, lev, 0, part, down),
            loc_copy(b, 4, down, 0, part, up),
            loc_copy(b, 5, up, part, part, down),
            loc_copy(b, 6, lev, 0, held, mate),
            loc_copy(b, 7, down, 0, held, mate),
            loc_copy(b, 8, up, 0, held, mate),
            loc_copy(b, 9, far, 0, held, mate),
        ])

    def ring_begin(b):
        for i in (0, 1, 2, 3, 6):
            remote.start(ring[b][i])

    def ring_forward(b):
        for first, then in ((0, 4), (1, 5), (2, 7), (3, 8)):
            remote.arrived(ring[b][first])
            remote.start(ring[b][then])

    def ring_finish(b):
        remote.arrived(ring[b][4])
        remote.arrived(ring[b][5])
        remote.start(ring[b][9])
        for i in (6, 7, 8, 9):
            remote.arrived(ring[b][i])

    a_copies = [[
        pltpu.make_async_remote_copy(
            src_ref=abuf.at[r, 0], dst_ref=abuf.at[r, k],
            send_sem=a_send.at[r, k], recv_sem=a_recv.at[r, k],
            device_id=(slab_peer[k], lev), device_id_type=MESH,
        ) if k else None for k in range(n_slab)] for r in range(2)]
    b_copies = [[
        pltpu.make_async_remote_copy(
            src_ref=bbuf.at[r, 0], dst_ref=bbuf.at[r, k],
            send_sem=b_send.at[r, k], recv_sem=b_recv.at[r, k],
            device_id=(slab, lev_peer[k]), device_id_type=MESH,
        ) if k else None for k in range(n_lev)] for r in range(2)]

    lane1 = lax.broadcasted_iota(jnp.int32, (1, 128), 1)
    low1 = lane1 < SLOTS

    def send_priors(r, cells, weights):
        for q in range(chunks):
            weighted = cells[:, 128 * q : 128 * (q + 1)] * weights[q]
            both = weighted + pltpu.roll(weighted, SLOTS, 1)
            abuf[r, 0, q] = jnp.where(low1, both[:half], both[half:])
        for k in slab_order:
            remote.start(a_copies[r][k])

    def band_statistics(r, values):
        for k in range(1, n_slab):
            remote.arrived(a_copies[r][k])
        for q in range(chunks):
            packed = abuf[r, 0, q]
            for k in range(1, n_slab):
                packed = packed + abuf[r, k, q]
            turned = pltpu.roll(packed, SLOTS, 1)
            prior = jnp.concatenate(
                [jnp.where(low1, packed, turned), jnp.where(low1, turned, packed)], axis=0
            )
            value, variance = values[q]
            mean = jnp.sum(prior, axis=0, keepdims=True) / float(members)
            deviation = prior - mean
            spread = jnp.sum(deviation * deviation, axis=0, keepdims=True) / (members - 1.0)
            total = spread + variance
            shrink = 1.0 / (1.0 + jnp.sqrt(variance / total))
            gain = ((value - mean) - deviation * shrink) / (total * (members - 1.0))
            bbuf[r, 0, q, pl.ds(0, members), :] = jnp.where(low1, deviation, gain).astype(BF16)
            high, mid, low = (x.astype(F32) for x in split3(mean))
            row = lax.broadcasted_iota(jnp.int32, (16, 128), 0)
            parts = jnp.where(row == 0, high, jnp.where(row == 1, mid, jnp.where(row == 2, low, 0.0)))
            bbuf[r, 0, q, pl.ds(members, 16), :] = parts.astype(BF16)
        for k in lev_order:
            remote.start(b_copies[r][k])

    def obs_order(found):
        band = column_of(found, 0)
        band_stack = count_at_least(band, 2, stack)
        band_core = band - 2.0 * band_stack
        away = (lev // 2).astype(F32) - band_stack
        away = jnp.where(away < 0.0, away + float(stack), away) * 2.0
        away = away + jnp.where(band_core == core.astype(F32), 0.0, 1.0)
        to_dev = []
        to_gain = []
        for k in range(n_lev):
            for q in range(chunks):
                chosen = (away == float(k)) & (found[1] == lane_slot + float(SLOTS * q))
                to_dev.append(jnp.where(chosen & first_half, 1.0, 0.0).astype(BF16))
                to_gain.append(jnp.where(chosen & ~first_half, 1.0, 0.0).astype(BF16))
        return jnp.concatenate(to_dev, axis=1), jnp.concatenate(to_gain, axis=1)

    def all_statistics(r, to_dev, to_gain):
        for k in range(1, n_lev):
            remote.arrived(b_copies[r][k])
        packed = jnp.concatenate(
            [bbuf[r, k, q] for k in range(n_lev) for q in range(chunks)], axis=1
        )
        dev = nt_dot(to_dev, packed)[:, :members].astype(BF16)
        gain = nt_dot(packed[:members], to_gain).astype(BF16)
        return dev, gain

    def all_means(r, to_dev):
        packed = jnp.concatenate(
            [bbuf[r, k, q, pl.ds(members, 16), :] for k in range(n_lev) for q in range(chunks)], axis=1
        )
        means = nt_dot(packed, to_dev)
        mean_out[pl.ds(r, 1), :] = means[0:1] + means[1:2] + means[2:3]

    def at(c):
        return pl.ds(pl.multiple_of(c * width, width), width)

    def regress(dev, gain):
        def step(c, carry):
            local = loc_first[:, :, at(c)].reshape(n_obs, width).astype(F32)
            for l in range(lev_rows):
                now = ens[l, :, at(c)]
                mean = jnp.sum(now, axis=0, keepdims=True) / float(members)
                centred = (now - mean).astype(BF16)
                cross = jnp.dot(dev, centred, preferred_element_type=F32)
                weight = jnp.tile(level_wide[l], (1, width // 128)) * local
                mixed = (weight * cross).astype(BF16)
                ens[l, :, at(c)] = now + jnp.dot(gain, mixed, preferred_element_type=F32)
            return carry

        lax.fori_loop(0, cols // width, step, 0)

    found0 = locate(0)
    places, inners = slot_places(found0)
    weights0 = slot_weights(found0)
    for copy in ens_copies:
        copy.wait()
    _, cells = gather_cells(places, inners)
    pl.semaphore_wait(barrier, n_lev + n_slab - 2)
    own_copies[0].wait()
    ring_begin(0)
    send_priors(0, cells, weights0)

    values0 = slot_values(found0)
    found1 = locate(1)
    places, inners = slot_places(found1)
    weights1 = slot_weights(found1)
    hot, now = gather_cells(places, inners)
    to_dev, to_gain = obs_order(found0)
    ring_forward(0)
    own_copies[1].wait()
    band_statistics(0, values0)
    for l in range(lev_rows):
        level_wide[l] = jnp.broadcast_to(column_of(found0, 7 + l), (n_obs, 128))
    level_out[...] = found1[0]
    ring_finish(0)

    weights = jnp.dot(loc_first[...].reshape(n_obs, cols), hot, preferred_element_type=F32)
    level_weight = jnp.zeros((n_obs, 128 * chunks), F32)
    for l in range(lev_rows):
        level_weight = jnp.where(inners == float(l), column_of(found0, 7 + l), level_weight)
    weights = level_weight * weights
    centred = (now - jnp.sum(now, axis=0, keepdims=True) / float(members)).astype(BF16)

    dev, gain = all_statistics(0, to_dev, to_gain)
    cross = jnp.dot(dev, centred, preferred_element_type=F32)
    mixed = (weights * cross).astype(BF16)
    now = now + jnp.dot(gain, mixed, preferred_element_type=F32)
    send_priors(1, now, weights1)
    ring_begin(1)

    crowd_out[0] = (jnp.maximum(found0[2], found1[2]) >= float(SLOTS * chunks)).astype(jnp.int32)
    all_means(0, to_dev)
    values1 = slot_values(found1)
    regress(dev, gain)
    to_dev, to_gain = obs_order(found1)
    ring_forward(1)
    band_statistics(1, values1)
    ring_finish(1)
    dev, gain = all_statistics(1, to_dev, to_gain)
    dev_out[...] = dev
    gain_out[...] = gain
    all_means(1, to_dev)
    remote.drain()


def run_filter(chunks, n_slab, n_lev, obs_cell, obs_value, obs_var, obs_frac, loc_level, ensemble, loc_column):
    members, lev_rows, cols = ensemble.shape
    n_obs = obs_cell.shape[1]
    held = loc_column.shape[1]
    width = WIDTH if cols % WIDTH == 0 else cols
    vmem = pl.BlockSpec(memory_space=pltpu.VMEM)
    hbm = pl.BlockSpec(memory_space=pltpu.HBM)
    dma = pltpu.SemaphoreType.DMA
    return pl.pallas_call(
        functools.partial(filter_kernel, chunks, n_slab, n_lev, width),
        out_shape=(
            pltpu.VMEM((lev_rows, members, cols), F32),
            pltpu.VMEM((n_lev, held, cols), BF16),
            pltpu.VMEM((n_obs, members), BF16),
            pltpu.VMEM((members, n_obs), BF16),
            pltpu.VMEM((n_obs, 128), F32),
            pltpu.VMEM((2, n_obs), F32),
            pltpu.SMEM((1,), jnp.int32),
        ),
        in_specs=[hbm] * 7,
        out_specs=(vmem,) * 6 + (pl.BlockSpec(memory_space=pltpu.SMEM),),
        scratch_shapes=[
            pltpu.VMEM((n_lev, held, cols), BF16),
            pltpu.VMEM(obs_cell.shape, jnp.int32),
            pltpu.VMEM(obs_cell.shape, F32),
            pltpu.VMEM(obs_cell.shape, F32),
            pltpu.VMEM(obs_cell.shape, F32),
            pltpu.VMEM(loc_level.shape, F32),
            pltpu.VMEM((2, n_slab, chunks, members // 2, 128), F32),
            pltpu.VMEM((2, n_lev, chunks, members + 16, 128), BF16),
            pltpu.VMEM((lev_rows, n_obs, 128), F32),
            dma((5,)),
            dma((lev_rows,)),
            dma((2,)),
            dma((2, n_slab)),
            dma((2, n_slab)),
            dma((2, n_lev)),
            dma((2, n_lev)),
            dma((2, 10)),
            dma((2, 10)),
        ],
        compiler_params=pltpu.CompilerParams(
            collective_id=chunks, has_side_effects=True, vmem_limit_bytes=VMEM_LIMIT
        ),
    )(*(pltpu.with_memory_space_constraint(x, pltpu.HBM) for x in (
        obs_cell, obs_value, obs_var, obs_frac, loc_level, ensemble, loc_column)))


def last_kernel(ens, loc, dev_ref, gain_ref, level_ref, mean_ref, out_hbm, mean_hbm, out, out_sem, mean_sem):
    lev_rows, members, cols = ens.shape
    n_obs = dev_ref.shape[0]
    dev = dev_ref[...]
    gain = gain_ref[...]
    copies = [pltpu.make_async_copy(mean_ref, mean_hbm, mean_sem)]
    copies[0].start()
    for l in range(lev_rows):
        now = ens[l]
        mean = jnp.sum(now, axis=0, keepdims=True) / float(members)
        centred = (now - mean).astype(BF16)
        cross = jnp.dot(dev, centred, preferred_element_type=F32)
        place = LEVEL_AT + l
        weight = level_ref[:, place : place + 1] * loc[...].reshape(n_obs, cols).astype(F32)
        mixed = (weight * cross).astype(BF16)
        out[l] = now + jnp.dot(gain, mixed, preferred_element_type=F32)
        copies.append(pltpu.make_async_copy(out.at[l], out_hbm.at[:, l, :], out_sem.at[l]))
        copies[l + 1].start()
    for copy in copies:
        copy.wait()


LEVEL_AT = 7
PIECES = 3
VMEM_LIMIT = 40 * 1024 * 1024
WIDTH = 2304
COND = True


def last_update(ens, loc, dev, gain, level, mean):
    lev_rows, members, cols = ens.shape
    vmem = pl.BlockSpec(memory_space=pltpu.VMEM)
    hbm = pl.BlockSpec(memory_space=pltpu.HBM)
    return pl.pallas_call(
        last_kernel,
        out_shape=(pltpu.HBM((members, lev_rows, cols), F32), pltpu.HBM(mean.shape, F32)),
        in_specs=[vmem] * 6,
        out_specs=(hbm, hbm),
        scratch_shapes=[
            pltpu.VMEM((lev_rows, members, cols), F32),
            pltpu.SemaphoreType.DMA((lev_rows,)),
            pltpu.SemaphoreType.DMA,
        ],
        compiler_params=pltpu.CompilerParams(vmem_limit_bytes=VMEM_LIMIT),
    )(*(pltpu.with_memory_space_constraint(x, pltpu.VMEM) for x in (ens, loc, dev, gain, level, mean)))


def on_device(n_slab, n_lev, ensemble, obs_cell, obs_value, obs_var, obs_frac, loc_column, loc_level):
    members, lev_rows, slab_cols = ensemble.shape
    n_obs = obs_cell.shape[1]
    operands = (obs_cell, obs_value, obs_var, obs_frac, jnp.swapaxes(loc_level, 1, 2), ensemble, loc_column)

    def whole(chunks):
        *state, crowd = run_filter(chunks, n_slab, n_lev, *operands)
        return (crowd[0], *last_update(*state))

    done = lax.while_loop(lambda state: state[0] != 0, lambda state: whole(3), whole(1))
    return done[1], done[2]


def solution(mesh):
    in_specs = (
        P(None, "lev", "slab"),
        P(),
        P(),
        P(),
        P(),
        P(None, "lev", "slab"),
        P(None, None, "lev"),
    )
    out_specs = (P(None, "lev", "slab"), P())
    return jax.shard_map(
        functools.partial(on_device, mesh.shape["slab"], mesh.shape["lev"]),
        mesh=mesh, in_specs=in_specs, out_specs=out_specs, check_vma=False,
    )
```

```python
import functools
import math

import jax
import jax.numpy as jnp
from jax import lax
from jax.experimental import pallas as pl
from jax.experimental.pallas import tpu as pltpu
from jax.sharding import PartitionSpec as P

MESH = pl.DeviceIdType.MESH
SLOTS = 64
F32 = jnp.float32
BF16 = jnp.bfloat16


def nt_dot(a, b):
    return lax.dot_general(a, b, (((1,), (1,)), ((), ())), preferred_element_type=F32)


def mean_of(packed, to_dev):
    parts = nt_dot(packed, to_dev)
    return parts[0:1] + parts[1:2] + parts[2:3]


def count_at_least(x, step, number):
    total = jnp.zeros_like(x)
    for k in range(1, number):
        total = total + jnp.where(x >= float(k * step), 1.0, 0.0)
    return total


def split3(x):
    high = x.astype(BF16)
    rest = x - high.astype(F32)
    mid = rest.astype(BF16)
    low = (rest - mid.astype(F32)).astype(BF16)
    return high, mid, low


class Tracker:
    def __init__(self):
        self.sends = []
        self.recvs = []

    def start(self, copy):
        copy.start()
        self.sends.append(copy)
        self.recvs.append(copy)

    def arrived(self, copy):
        copy.wait_recv()
        self.recvs = [c for c in self.recvs if c is not copy]

    def drain(self):
        for copy in self.recvs:
            copy.wait_recv()
        for copy in self.sends:
            copy.wait_send()


def filter_kernel(
    chunks, n_slab, n_lev, width,
    cell_hbm, value_hbm, var_hbm, frac_hbm, level_hbm, ens_hbm, loc_hbm,
    ens, centred_out, weight_out, dev_out, gain_out, place_out, packed_out, mean_out, crowd_out,
    loc_first, loc_last, cell_ref, value_ref, var_ref, frac_ref, level_ref, abuf, bbuf, level_wide,
    small_sem, ens_sem, own_sem, a_send, a_recv, b_send, b_recv, l_send, l_recv,
):
    slab = lax.axis_index("slab")
    lev = lax.axis_index("lev")
    lev_rows, members, cols = ens.shape
    n_obs = cell_ref.shape[1]
    loc = (loc_first, loc_last)
    total_cols = cols * n_slab
    half = members // 2
    remote = Tracker()

    barrier = pltpu.get_barrier_semaphore()
    side = math.isqrt(n_slab)
    stack = n_lev // 2

    def around(k, n):
        return min(k, n - k)

    slab_peer = [
        lax.rem(slab // side + k // side, side) * side + lax.rem(lax.rem(slab, side) + k % side, side)
        for k in range(n_slab)
    ]
    core = lax.rem(lev, 2)
    lev_peer = [
        lax.rem(lev // 2 + k // 2, stack) * 2 + (1 - core if k % 2 else core) for k in range(n_lev)
    ]
    slab_order = sorted(
        range(1, n_slab), key=lambda k: -around(k // side, side) - around(k % side, side)
    )
    lev_order = sorted(range(1, n_lev), key=lambda k: -around(k // 2, stack))
    for k in slab_order:
        pl.semaphore_signal(barrier, inc=1, device_id=(slab_peer[k], lev), device_id_type=MESH)
    for k in lev_order:
        pl.semaphore_signal(barrier, inc=1, device_id=(slab, lev_peer[k]), device_id_type=MESH)
    small_copies = [
        pltpu.make_async_copy(source, target, small_sem.at[i])
        for i, (source, target) in enumerate([
            (cell_hbm, cell_ref), (value_hbm, value_ref), (var_hbm, var_ref),
            (frac_hbm, frac_ref), (level_hbm, level_ref),
        ])
    ]
    for copy in small_copies:
        copy.start()
    ens_copies = [
        pltpu.make_async_copy(ens_hbm.at[:, l, :], ens.at[l], ens_sem.at[l])
        for l in range(lev_rows)
    ]
    for copy in ens_copies:
        copy.start()
    own_copies = [
        pltpu.make_async_copy(loc_hbm.at[b], loc[b].at[lev], own_sem.at[b]) for b in range(2)
    ]
    for copy in own_copies:
        copy.start()

    for copy in small_copies:
        copy.wait()

    slab_f = slab.astype(F32)
    lev_f = lev.astype(F32)
    lane = lax.broadcasted_iota(jnp.int32, (n_obs, 128), 1)
    lane_slot = jnp.where(lane < SLOTS, lane, lane - SLOTS).astype(F32)
    first_half = lane < SLOTS

    def locate(b):
        cell = cell_ref[pl.ds(b, 1), :].astype(F32)
        level = count_at_least(cell, total_cols, n_lev * lev_rows)
        column = cell - level * float(total_cols)
        later = column + 1.0
        later = jnp.where(later >= float(total_cols), 0.0, later)
        band = count_at_least(level, lev_rows, n_lev)
        inner = level - band * float(lev_rows)
        places = []
        for where_at in (column, later):
            in_slab = count_at_least(where_at, cols, n_slab)
            place = where_at - in_slab * float(cols) + 1.0
            places.append(jnp.where(in_slab == slab_f, place, 0.0))
        flat = [band, places[0], places[1], inner,
                value_ref[pl.ds(b, 1), :], var_ref[pl.ds(b, 1), :], frac_ref[pl.ds(b, 1), :]]
        flat = flat + [level_ref[b, pl.ds(l, 1), :] for l in range(lev_rows)]
        table = jnp.concatenate(flat + [jnp.zeros((128 - len(flat), n_obs), F32)], axis=0).T
        other = lax.broadcasted_iota(jnp.int32, (n_obs, n_obs), 1)
        mine = lax.broadcasted_iota(jnp.int32, (n_obs, n_obs), 0)
        earlier = (table[:, 0:1] == band) & (other < mine)
        rank = jnp.sum(jnp.where(earlier, 1.0, 0.0), axis=1, keepdims=True)
        return table, rank, jnp.max(rank)

    def column_of(found, i):
        return found[0][:, i : i + 1]

    def picked(found, q, x):
        chosen = (column_of(found, 0) == lev_f) & (found[1] == lane_slot + float(SLOTS * q))
        return jnp.sum(jnp.where(chosen, x, 0.0), axis=0, keepdims=True)

    def slot_places(found):
        place = jnp.where(first_half, column_of(found, 1), column_of(found, 2))
        inner = jnp.broadcast_to(column_of(found, 3), (n_obs, 128))
        return (
            jnp.concatenate([picked(found, q, place) - 1.0 for q in range(chunks)], axis=1),
            jnp.concatenate([picked(found, q, inner) for q in range(chunks)], axis=1),
        )

    def slot_weights(found):
        frac = column_of(found, 6)
        weight = jnp.where(first_half, 1.0 - frac, frac)
        return [picked(found, q, weight) for q in range(chunks)]

    def slot_values(found):
        pairs = []
        for q in range(chunks):
            value = picked(found, q, column_of(found, 4))
            var = picked(found, q, column_of(found, 5) - 1.0) + 1.0
            pairs.append((value, var))
        return pairs

    def gather_cells(places, inners):
        index = lax.broadcasted_iota(jnp.int32, (cols, 128 * chunks), 0).astype(F32)
        hot = jnp.where(index == places, 1.0, 0.0).astype(BF16)
        cells = jnp.zeros((members, 128 * chunks), F32)
        for l in range(lev_rows):
            left = jnp.concatenate(split3(ens[l])[:PIECES], axis=0)
            found = jnp.dot(left, hot, preferred_element_type=F32)
            total = found[:members]
            for i in range(1, PIECES):
                total = total + found[i * members : (i + 1) * members]
            cells = jnp.where(inners == float(l), total, cells)
        return hot, jnp.where(places >= 0.0, cells, 0.0)

    def loc_copy(b, which, holder, start, count, target):
        piece = loc[b].at[holder, pl.ds(start, count)]
        return pltpu.make_async_remote_copy(
            src_ref=piece, dst_ref=piece,
            send_sem=l_send.at[b, which], recv_sem=l_recv.at[b, which],
            device_id=(slab, target), device_id_type=MESH,
        )

    up = lax.rem(lev + 2, n_lev)
    down = lax.rem(lev + n_lev - 2, n_lev)
    far = lax.rem(lev + 4, n_lev)
    mate = lev + 1 - 2 * lax.rem(lev, 2)
    held = loc_first.shape[1]
    part = held // 2
    ring = []
    for b in range(2):
        ring.append([
            loc_copy(b, 0, lev, 0, part, up),
            loc_copy(b, 1, lev, part, part, down),
            loc_copy(b, 2, lev, part, part, up),
            loc_copy(b, 3, lev, 0, part, down),
            loc_copy(b, 4, down, 0, part, up),
            loc_copy(b, 5, up, part, part, down),
            loc_copy(b, 6, lev, 0, held, mate),
            loc_copy(b, 7, down, 0, held, mate),
            loc_copy(b, 8, up, 0, held, mate),
            loc_copy(b, 9, far, 0, held, mate),
        ])

    def ring_begin(b):
        for i in (0, 1, 2, 3, 6):
            remote.start(ring[b][i])

    def ring_forward(b):
        for first, then in ((0, 4), (1, 5), (2, 7), (3, 8)):
            remote.arrived(ring[b][first])
            remote.start(ring[b][then])

    def ring_finish(b):
        remote.arrived(ring[b][4])
        remote.arrived(ring[b][5])
        remote.start(ring[b][9])
        for i in (6, 7, 8, 9):
            remote.arrived(ring[b][i])

    a_copies = [[
        pltpu.make_async_remote_copy(
            src_ref=abuf.at[r, 0], dst_ref=abuf.at[r, k],
            send_sem=a_send.at[r, k], recv_sem=a_recv.at[r, k],
            device_id=(slab_peer[k], lev), device_id_type=MESH,
        ) if k else None for k in range(n_slab)] for r in range(2)]
    b_copies = [[
        pltpu.make_async_remote_copy(
            src_ref=bbuf.at[r, 0], dst_ref=bbuf.at[r, k],
            send_sem=b_send.at[r, k], recv_sem=b_recv.at[r, k],
            device_id=(slab, lev_peer[k]), device_id_type=MESH,
        ) if k else None for k in range(n_lev)] for r in range(2)]

    lane1 = lax.broadcasted_iota(jnp.int32, (1, 128), 1)
    low1 = lane1 < SLOTS

    def send_priors(r, cells, weights):
        for q in range(chunks):
            weighted = cells[:, 128 * q : 128 * (q + 1)] * weights[q]
            both = weighted + pltpu.roll(weighted, SLOTS, 1)
            abuf[r, 0, q] = jnp.where(low1, both[:half], both[half:])
        for k in slab_order:
            remote.start(a_copies[r][k])

    def band_statistics(r, values):
        for k in range(1, n_slab):
            remote.arrived(a_copies[r][k])
        for q in range(chunks):
            packed = abuf[r, 0, q]
            for k in range(1, n_slab):
                packed = packed + abuf[r, k, q]
            turned = pltpu.roll(packed, SLOTS, 1)
            prior = jnp.concatenate(
                [jnp.where(low1, packed, turned), jnp.where(low1, turned, packed)], axis=0
            )
            value, variance = values[q]
            mean = jnp.sum(prior, axis=0, keepdims=True) / float(members)
            deviation = prior - mean
            spread = jnp.sum(deviation * deviation, axis=0, keepdims=True) / (members - 1.0)
            total = spread + variance
            shrink = 1.0 / (1.0 + jnp.sqrt(variance / total))
            gain = ((value - mean) - deviation * shrink) / (total * (members - 1.0))
            bbuf[r, 0, q, pl.ds(0, members), :] = jnp.where(low1, deviation, gain).astype(BF16)
            high, mid, low = (x.astype(F32) for x in split3(mean))
            row = lax.broadcasted_iota(jnp.int32, (16, 128), 0)
            parts = jnp.where(row == 0, high, jnp.where(row == 1, mid, jnp.where(row == 2, low, 0.0)))
            bbuf[r, 0, q, pl.ds(members, 16), :] = parts.astype(BF16)
        for k in lev_order:
            remote.start(b_copies[r][k])

    def obs_order(found):
        band = column_of(found, 0)
        band_stack = count_at_least(band, 2, stack)
        band_core = band - 2.0 * band_stack
        away = (lev // 2).astype(F32) - band_stack
        away = jnp.where(away < 0.0, away + float(stack), away) * 2.0
        away = away + jnp.where(band_core == core.astype(F32), 0.0, 1.0)
        to_dev = []
        to_gain = []
        for k in range(n_lev):
            for q in range(chunks):
                chosen = (away == float(k)) & (found[1] == lane_slot + float(SLOTS * q))
                to_dev.append(jnp.where(chosen & first_half, 1.0, 0.0).astype(BF16))
                to_gain.append(jnp.where(chosen & ~first_half, 1.0, 0.0).astype(BF16))
        return jnp.concatenate(to_dev, axis=1), jnp.concatenate(to_gain, axis=1)

    def all_statistics(r, to_dev, to_gain):
        for k in range(1, n_lev):
            remote.arrived(b_copies[r][k])
        packed = jnp.concatenate(
            [bbuf[r, k, q] for k in range(n_lev) for q in range(chunks)], axis=1
        )
        dev = nt_dot(to_dev, packed)[:, :members].astype(BF16)
        gain = nt_dot(packed[:members], to_gain).astype(BF16)
        return dev, gain

    def mean_rows(r):
        return jnp.concatenate(
            [bbuf[r, k, q, pl.ds(members, 16), :] for k in range(n_lev) for q in range(chunks)], axis=1
        )

    def at(c):
        return pl.ds(pl.multiple_of(c * width, width), width)

    def regress(dev, gain):
        def step(c, carry):
            local = loc_first[:, :, at(c)].reshape(n_obs, width).astype(F32)
            for l in range(lev_rows):
                now = ens[l, :, at(c)]
                mean = jnp.sum(now, axis=0, keepdims=True) / float(members)
                centred = (now - mean).astype(BF16)
                cross = jnp.dot(dev, centred, preferred_element_type=F32)
                weight = jnp.tile(level_wide[l], (1, width // 128)) * local
                mixed = (weight * cross).astype(BF16)
                now = now + jnp.dot(gain, mixed, preferred_element_type=F32)
                ens[l, :, at(c)] = now
                mean = jnp.sum(now, axis=0, keepdims=True) / float(members)
                centred_out[l, :, at(c)] = (now - mean).astype(BF16)
            return carry

        lax.fori_loop(0, cols // width, step, 0)

    found0 = locate(0)
    places, inners = slot_places(found0)
    weights0 = slot_weights(found0)
    for copy in ens_copies:
        copy.wait()
    _, cells = gather_cells(places, inners)
    pl.semaphore_wait(barrier, n_lev + n_slab - 2)
    own_copies[0].wait()
    ring_begin(0)
    send_priors(0, cells, weights0)

    values0 = slot_values(found0)
    found1 = locate(1)
    places, inners = slot_places(found1)
    weights1 = slot_weights(found1)
    hot, now = gather_cells(places, inners)
    to_dev, to_gain = obs_order(found0)
    ring_forward(0)
    own_copies[1].wait()
    band_statistics(0, values0)
    for l in range(lev_rows):
        level_wide[l] = jnp.broadcast_to(column_of(found0, 7 + l), (n_obs, 128))
    ring_finish(0)

    weights = jnp.dot(loc_first[...].reshape(n_obs, cols), hot, preferred_element_type=F32)
    level_weight = jnp.zeros((n_obs, 128 * chunks), F32)
    for l in range(lev_rows):
        level_weight = jnp.where(inners == float(l), column_of(found0, 7 + l), level_weight)
    weights = level_weight * weights
    centred = (now - jnp.sum(now, axis=0, keepdims=True) / float(members)).astype(BF16)

    dev, gain = all_statistics(0, to_dev, to_gain)
    cross = jnp.dot(dev, centred, preferred_element_type=F32)
    mixed = (weights * cross).astype(BF16)
    now = now + jnp.dot(gain, mixed, preferred_element_type=F32)
    send_priors(1, now, weights1)
    ring_begin(1)

    crowd_out[0] = (jnp.maximum(found0[2], found1[2]) >= float(SLOTS * chunks)).astype(jnp.int32)
    mean_out[...] = mean_of(mean_rows(0), to_dev)
    values1 = slot_values(found1)
    regress(dev, gain)
    to_dev, to_gain = obs_order(found1)
    place_out[...] = to_dev
    ring_forward(1)
    band_statistics(1, values1)
    ring_finish(1)
    local = loc_last[...].reshape(n_obs, cols).astype(F32)
    for l in range(lev_rows):
        weight_out[l] = column_of(found1, 7 + l) * local
    dev, gain = all_statistics(1, to_dev, to_gain)
    dev_out[...] = dev
    gain_out[...] = gain
    packed_out[...] = mean_rows(1)
    remote.drain()


def run_filter(chunks, n_slab, n_lev, obs_cell, obs_value, obs_var, obs_frac, loc_level, ensemble, loc_column):
    members, lev_rows, cols = ensemble.shape
    n_obs = obs_cell.shape[1]
    held = loc_column.shape[1]
    width = WIDTH if cols % WIDTH == 0 else cols
    vmem = pl.BlockSpec(memory_space=pltpu.VMEM)
    hbm = pl.BlockSpec(memory_space=pltpu.HBM)
    dma = pltpu.SemaphoreType.DMA
    return pl.pallas_call(
        functools.partial(filter_kernel, chunks, n_slab, n_lev, width),
        out_shape=(
            pltpu.VMEM((lev_rows, members, cols), F32),
            pltpu.VMEM((lev_rows, members, cols), BF16),
            pltpu.VMEM((lev_rows, n_obs, cols), F32),
            pltpu.VMEM((n_obs, members), BF16),
            pltpu.VMEM((members, n_obs), BF16),
            pltpu.VMEM((n_obs, n_lev * chunks * 128), BF16),
            pltpu.VMEM((16, n_lev * chunks * 128), BF16),
            pltpu.VMEM((1, n_obs), F32),
            pltpu.SMEM((1,), jnp.int32),
        ),
        in_specs=[hbm] * 7,
        out_specs=(vmem,) * 8 + (pl.BlockSpec(memory_space=pltpu.SMEM),),
        scratch_shapes=[
            pltpu.VMEM((n_lev, held, cols), BF16),
            pltpu.VMEM((n_lev, held, cols), BF16),
            pltpu.VMEM(obs_cell.shape, jnp.int32),
            pltpu.VMEM(obs_cell.shape, F32),
            pltpu.VMEM(obs_cell.shape, F32),
            pltpu.VMEM(obs_cell.shape, F32),
            pltpu.VMEM(loc_level.shape, F32),
            pltpu.VMEM((2, n_slab, chunks, members // 2, 128), F32),
            pltpu.VMEM((2, n_lev, chunks, members + 16, 128), BF16),
            pltpu.VMEM((lev_rows, n_obs, 128), F32),
            dma((5,)),
            dma((lev_rows,)),
            dma((2,)),
            dma((2, n_slab)),
            dma((2, n_slab)),
            dma((2, n_lev)),
            dma((2, n_lev)),
            dma((2, 10)),
            dma((2, 10)),
        ],
        compiler_params=pltpu.CompilerParams(
            collective_id=chunks, has_side_effects=True, vmem_limit_bytes=VMEM_LIMIT
        ),
    )(*(pltpu.with_memory_space_constraint(x, pltpu.HBM) for x in (
        obs_cell, obs_value, obs_var, obs_frac, loc_level, ensemble, loc_column)))


def last_kernel(
    ens, centred, weight, dev_ref, gain_ref, place_ref, packed_ref, mean_ref,
    out_hbm, mean_hbm, out, mean, out_sem, mean_sem,
):
    lev_rows = ens.shape[0]
    dev = dev_ref[...]
    gain = gain_ref[...]
    copies = []
    for l in range(lev_rows):
        cross = jnp.dot(dev, centred[l], preferred_element_type=F32)
        mixed = (weight[l] * cross).astype(BF16)
        out[l] = ens[l] + jnp.dot(gain, mixed, preferred_element_type=F32)
        copies.append(pltpu.make_async_copy(out.at[l], out_hbm.at[:, l, :], out_sem.at[l]))
        copies[l].start()
        if l == MEAN_AFTER:
            mean[pl.ds(0, 1), :] = mean_ref[...]
            mean[pl.ds(1, 1), :] = mean_of(packed_ref[...], place_ref[...])
            mean_copy = pltpu.make_async_copy(mean, mean_hbm, mean_sem)
            mean_copy.start()
    for copy in copies:
        copy.wait()
    mean_copy.wait()


MEAN_AFTER = 3
PIECES = 3
VMEM_LIMIT = 40 * 1024 * 1024
WIDTH = 2304
COND = True


def last_update(ens, *rest):
    lev_rows, members, cols = ens.shape
    means = (2, rest[-1].shape[1])
    vmem = pl.BlockSpec(memory_space=pltpu.VMEM)
    hbm = pl.BlockSpec(memory_space=pltpu.HBM)
    return pl.pallas_call(
        last_kernel,
        out_shape=(pltpu.HBM((members, lev_rows, cols), F32), pltpu.HBM(means, F32)),
        in_specs=[vmem] * 8,
        out_specs=(hbm, hbm),
        scratch_shapes=[
            pltpu.VMEM((lev_rows, members, cols), F32),
            pltpu.VMEM(means, F32),
            pltpu.SemaphoreType.DMA((lev_rows,)),
            pltpu.SemaphoreType.DMA,
        ],
        compiler_params=pltpu.CompilerParams(vmem_limit_bytes=VMEM_LIMIT),
    )(*(pltpu.with_memory_space_constraint(x, pltpu.VMEM) for x in (ens, *rest)))


def on_device(n_slab, n_lev, ensemble, obs_cell, obs_value, obs_var, obs_frac, loc_column, loc_level):
    members, lev_rows, slab_cols = ensemble.shape
    n_obs = obs_cell.shape[1]
    operands = (obs_cell, obs_value, obs_var, obs_frac, jnp.swapaxes(loc_level, 1, 2), ensemble, loc_column)

    def whole(chunks):
        *state, crowd = run_filter(chunks, n_slab, n_lev, *operands)
        return (crowd[0], *last_update(*state))

    done = lax.while_loop(lambda state: state[0] != 0, lambda state: whole(3), whole(1))
    return done[1], done[2]


def solution(mesh):
    in_specs = (
        P(None, "lev", "slab"),
        P(),
        P(),
        P(),
        P(),
        P(None, "lev", "slab"),
        P(None, None, "lev"),
    )
    out_specs = (P(None, "lev", "slab"), P())
    return jax.shard_map(
        functools.partial(on_device, mesh.shape["slab"], mesh.shape["lev"]),
        mesh=mesh, in_specs=in_specs, out_specs=out_specs, check_vma=False,
    )
```

```python
import functools
import math

import jax
import jax.numpy as jnp
from jax import lax
from jax.experimental import pallas as pl
from jax.experimental.pallas import tpu as pltpu
from jax.sharding import PartitionSpec as P

MESH = pl.DeviceIdType.MESH
SLOTS = 64
F32 = jnp.float32
BF16 = jnp.bfloat16


def nt_dot(a, b):
    return lax.dot_general(a, b, (((1,), (1,)), ((), ())), preferred_element_type=F32)


def mean_of(packed, to_dev):
    parts = nt_dot(packed, to_dev)
    return parts[0:1] + parts[1:2] + parts[2:3]


def count_at_least(x, step, number):
    total = jnp.zeros_like(x)
    for k in range(1, number):
        total = total + jnp.where(x >= float(k * step), 1.0, 0.0)
    return total


def split3(x):
    high = x.astype(BF16)
    rest = x - high.astype(F32)
    mid = rest.astype(BF16)
    low = (rest - mid.astype(F32)).astype(BF16)
    return high, mid, low


class Tracker:
    def __init__(self):
        self.sends = []
        self.recvs = []

    def start(self, copy):
        copy.start()
        self.sends.append(copy)
        self.recvs.append(copy)

    def arrived(self, copy):
        copy.wait_recv()
        self.recvs = [c for c in self.recvs if c is not copy]

    def drain(self):
        for copy in self.recvs:
            copy.wait_recv()
        for copy in self.sends:
            copy.wait_send()


def filter_kernel(
    chunks, n_slab, n_lev, width,
    cell_hbm, value_hbm, var_hbm, frac_hbm, level_hbm, ens_hbm, loc_hbm,
    ens, centred_out, weight_out, dev_out, gain_out, place_out, packed_out, mean_out, crowd_out,
    loc_first, loc_last, cell_ref, value_ref, var_ref, frac_ref, level_ref, abuf, bbuf, level_wide,
    small_sem, ens_sem, own_sem, a_send, a_recv, b_send, b_recv, l_send, l_recv,
):
    slab = lax.axis_index("slab")
    lev = lax.axis_index("lev")
    lev_rows, members, cols = ens.shape
    n_obs = cell_ref.shape[1]
    loc = (loc_first, loc_last)
    total_cols = cols * n_slab
    half = members // 2
    remote = Tracker()

    barrier = pltpu.get_barrier_semaphore()
    side = math.isqrt(n_slab)
    stack = n_lev // 2

    def around(k, n):
        return min(k, n - k)

    slab_peer = [
        lax.rem(slab // side + k // side, side) * side + lax.rem(lax.rem(slab, side) + k % side, side)
        for k in range(n_slab)
    ]
    core = lax.rem(lev, 2)
    lev_peer = [
        lax.rem(lev // 2 + k // 2, stack) * 2 + (1 - core if k % 2 else core) for k in range(n_lev)
    ]
    slab_order = sorted(
        range(1, n_slab), key=lambda k: -around(k // side, side) - around(k % side, side)
    )
    lev_order = sorted(range(1, n_lev), key=lambda k: -around(k // 2, stack))
    for k in slab_order:
        pl.semaphore_signal(barrier, inc=1, device_id=(slab_peer[k], lev), device_id_type=MESH)
    for k in lev_order:
        pl.semaphore_signal(barrier, inc=1, device_id=(slab, lev_peer[k]), device_id_type=MESH)
    small_copies = [
        pltpu.make_async_copy(source, target, small_sem.at[i])
        for i, (source, target) in enumerate([
            (cell_hbm, cell_ref), (value_hbm, value_ref), (var_hbm, var_ref),
            (frac_hbm, frac_ref), (level_hbm, level_ref),
        ])
    ]
    for copy in small_copies:
        copy.start()
    ens_copies = [
        pltpu.make_async_copy(ens_hbm.at[:, l, :], ens.at[l], ens_sem.at[l])
        for l in range(lev_rows)
    ]
    for copy in ens_copies:
        copy.start()
    own_copies = [
        pltpu.make_async_copy(loc_hbm.at[b], loc[b].at[lev], own_sem.at[b]) for b in range(2)
    ]
    for copy in own_copies:
        copy.start()

    for copy in small_copies:
        copy.wait()

    slab_f = slab.astype(F32)
    lev_f = lev.astype(F32)
    lane = lax.broadcasted_iota(jnp.int32, (n_obs, 128), 1)
    lane_slot = jnp.where(lane < SLOTS, lane, lane - SLOTS).astype(F32)
    first_half = lane < SLOTS

    def locate(b):
        cell = cell_ref[pl.ds(b, 1), :].astype(F32)
        level = count_at_least(cell, total_cols, n_lev * lev_rows)
        column = cell - level * float(total_cols)
        later = column + 1.0
        later = jnp.where(later >= float(total_cols), 0.0, later)
        band = count_at_least(level, lev_rows, n_lev)
        inner = level - band * float(lev_rows)
        places = []
        for where_at in (column, later):
            in_slab = count_at_least(where_at, cols, n_slab)
            place = where_at - in_slab * float(cols) + 1.0
            places.append(jnp.where(in_slab == slab_f, place, 0.0))
        flat = [band, places[0], places[1], inner,
                value_ref[pl.ds(b, 1), :], var_ref[pl.ds(b, 1), :], frac_ref[pl.ds(b, 1), :]]
        flat = flat + [level_ref[b, pl.ds(l, 1), :] for l in range(lev_rows)]
        table = jnp.concatenate(flat + [jnp.zeros((128 - len(flat), n_obs), F32)], axis=0).T
        other = lax.broadcasted_iota(jnp.int32, (n_obs, n_obs), 1)
        mine = lax.broadcasted_iota(jnp.int32, (n_obs, n_obs), 0)
        earlier = (table[:, 0:1] == band) & (other < mine)
        rank = jnp.sum(jnp.where(earlier, 1.0, 0.0), axis=1, keepdims=True)
        return table, rank, jnp.max(rank)

    def column_of(found, i):
        return found[0][:, i : i + 1]

    def picked(found, q, x):
        chosen = (column_of(found, 0) == lev_f) & (found[1] == lane_slot + float(SLOTS * q))
        return jnp.sum(jnp.where(chosen, x, 0.0), axis=0, keepdims=True)

    def slot_places(found):
        place = jnp.where(first_half, column_of(found, 1), column_of(found, 2))
        inner = jnp.broadcast_to(column_of(found, 3), (n_obs, 128))
        return (
            jnp.concatenate([picked(found, q, place) - 1.0 for q in range(chunks)], axis=1),
            jnp.concatenate([picked(found, q, inner) for q in range(chunks)], axis=1),
        )

    def slot_weights(found):
        frac = column_of(found, 6)
        weight = jnp.where(first_half, 1.0 - frac, frac)
        return [picked(found, q, weight) for q in range(chunks)]

    def slot_values(found):
        pairs = []
        for q in range(chunks):
            value = picked(found, q, column_of(found, 4))
            var = picked(found, q, column_of(found, 5) - 1.0) + 1.0
            pairs.append((value, var))
        return pairs

    def gather_cells(places, inners, arriving=None):
        index = lax.broadcasted_iota(jnp.int32, (cols, 128 * chunks), 0).astype(F32)
        hot = jnp.where(index == places, 1.0, 0.0).astype(BF16)
        cells = jnp.zeros((members, 128 * chunks), F32)
        for l in range(lev_rows):
            if arriving is not None:
                arriving[l].wait()
            left = jnp.concatenate(split3(ens[l])[:PIECES], axis=0)
            found = jnp.dot(left, hot, preferred_element_type=F32)
            total = found[:members]
            for i in range(1, PIECES):
                total = total + found[i * members : (i + 1) * members]
            cells = jnp.where(inners == float(l), total, cells)
        return hot, jnp.where(places >= 0.0, cells, 0.0)

    def loc_copy(b, which, holder, start, count, target):
        piece = loc[b].at[holder, pl.ds(start, count)]
        return pltpu.make_async_remote_copy(
            src_ref=piece, dst_ref=piece,
            send_sem=l_send.at[b, which], recv_sem=l_recv.at[b, which],
            device_id=(slab, target), device_id_type=MESH,
        )

    up = lax.rem(lev + 2, n_lev)
    down = lax.rem(lev + n_lev - 2, n_lev)
    far = lax.rem(lev + 4, n_lev)
    mate = lev + 1 - 2 * lax.rem(lev, 2)
    held = loc_first.shape[1]
    part = held // 2
    ring = []
    for b in range(2):
        ring.append([
            loc_copy(b, 0, lev, 0, part, up),
            loc_copy(b, 1, lev, part, part, down),
            loc_copy(b, 2, lev, part, part, up),
            loc_copy(b, 3, lev, 0, part, down),
            loc_copy(b, 4, down, 0, part, up),
            loc_copy(b, 5, up, part, part, down),
            loc_copy(b, 6, lev, 0, held, mate),
            loc_copy(b, 7, down, 0, held, mate),
            loc_copy(b, 8, up, 0, held, mate),
            loc_copy(b, 9, far, 0, held, mate),
        ])

    def ring_begin(b):
        for i in (0, 1, 2, 3, 6):
            remote.start(ring[b][i])

    def ring_forward(b):
        for first, then in ((0, 4), (1, 5), (2, 7), (3, 8)):
            remote.arrived(ring[b][first])
            remote.start(ring[b][then])

    def ring_finish(b):
        remote.arrived(ring[b][4])
        remote.arrived(ring[b][5])
        remote.start(ring[b][9])
        for i in (6, 7, 8, 9):
            remote.arrived(ring[b][i])

    a_copies = [[
        pltpu.make_async_remote_copy(
            src_ref=abuf.at[r, 0], dst_ref=abuf.at[r, k],
            send_sem=a_send.at[r, k], recv_sem=a_recv.at[r, k],
            device_id=(slab_peer[k], lev), device_id_type=MESH,
        ) if k else None for k in range(n_slab)] for r in range(2)]
    b_copies = [[
        pltpu.make_async_remote_copy(
            src_ref=bbuf.at[r, 0], dst_ref=bbuf.at[r, k],
            send_sem=b_send.at[r, k], recv_sem=b_recv.at[r, k],
            device_id=(slab, lev_peer[k]), device_id_type=MESH,
        ) if k else None for k in range(n_lev)] for r in range(2)]

    lane1 = lax.broadcasted_iota(jnp.int32, (1, 128), 1)
    low1 = lane1 < SLOTS

    def send_priors(r, cells, weights):
        for q in range(chunks):
            weighted = cells[:, 128 * q : 128 * (q + 1)] * weights[q]
            both = weighted + pltpu.roll(weighted, SLOTS, 1)
            abuf[r, 0, q] = jnp.where(low1, both[:half], both[half:])
        for k in slab_order:
            remote.start(a_copies[r][k])

    def band_statistics(r, values):
        for k in range(1, n_slab):
            remote.arrived(a_copies[r][k])
        for q in range(chunks):
            packed = abuf[r, 0, q]
            for k in range(1, n_slab):
                packed = packed + abuf[r, k, q]
            turned = pltpu.roll(packed, SLOTS, 1)
            prior = jnp.concatenate(
                [jnp.where(low1, packed, turned), jnp.where(low1, turned, packed)], axis=0
            )
            value, variance = values[q]
            mean = jnp.sum(prior, axis=0, keepdims=True) / float(members)
            deviation = prior - mean
            spread = jnp.sum(deviation * deviation, axis=0, keepdims=True) / (members - 1.0)
            total = spread + variance
            shrink = 1.0 / (1.0 + jnp.sqrt(variance / total))
            gain = ((value - mean) - deviation * shrink) / (total * (members - 1.0))
            bbuf[r, 0, q, pl.ds(0, members), :] = jnp.where(low1, deviation, gain).astype(BF16)
            high, mid, low = (x.astype(F32) for x in split3(mean))
            row = lax.broadcasted_iota(jnp.int32, (16, 128), 0)
            parts = jnp.where(row == 0, high, jnp.where(row == 1, mid, jnp.where(row == 2, low, 0.0)))
            bbuf[r, 0, q, pl.ds(members, 16), :] = parts.astype(BF16)
        for k in lev_order:
            remote.start(b_copies[r][k])

    def obs_order(found):
        band = column_of(found, 0)
        band_stack = count_at_least(band, 2, stack)
        band_core = band - 2.0 * band_stack
        away = (lev // 2).astype(F32) - band_stack
        away = jnp.where(away < 0.0, away + float(stack), away) * 2.0
        away = away + jnp.where(band_core == core.astype(F32), 0.0, 1.0)
        to_dev = []
        to_gain = []
        for k in range(n_lev):
            for q in range(chunks):
                chosen = (away == float(k)) & (found[1] == lane_slot + float(SLOTS * q))
                to_dev.append(jnp.where(chosen & first_half, 1.0, 0.0).astype(BF16))
                to_gain.append(jnp.where(chosen & ~first_half, 1.0, 0.0).astype(BF16))
        return jnp.concatenate(to_dev, axis=1), jnp.concatenate(to_gain, axis=1)

    def all_statistics(r, to_dev, to_gain):
        for k in range(1, n_lev):
            remote.arrived(b_copies[r][k])
        packed = jnp.concatenate(
            [bbuf[r, k, q] for k in range(n_lev) for q in range(chunks)], axis=1
        )
        dev = nt_dot(to_dev, packed)[:, :members].astype(BF16)
        gain = nt_dot(packed[:members], to_gain).astype(BF16)
        return dev, gain

    def mean_rows(r):
        return jnp.concatenate(
            [bbuf[r, k, q, pl.ds(members, 16), :] for k in range(n_lev) for q in range(chunks)], axis=1
        )

    def at(c):
        return pl.ds(pl.multiple_of(c * width, width), width)

    def regress(dev, gain):
        def step(c, carry):
            local = loc_first[:, :, at(c)].reshape(n_obs, width).astype(F32)
            for l in range(lev_rows):
                now = ens[l, :, at(c)]
                mean = jnp.sum(now, axis=0, keepdims=True) / float(members)
                centred = (now - mean).astype(BF16)
                cross = jnp.dot(dev, centred, preferred_element_type=F32)
                weight = jnp.tile(level_wide[l], (1, width // 128)) * local
                mixed = (weight * cross).astype(BF16)
                now = now + jnp.dot(gain, mixed, preferred_element_type=F32)
                ens[l, :, at(c)] = now
                mean = jnp.sum(now, axis=0, keepdims=True) / float(members)
                centred_out[l, :, at(c)] = (now - mean).astype(BF16)
            return carry

        lax.fori_loop(0, cols // width, step, 0)

    found0 = locate(0)
    places, inners = slot_places(found0)
    weights0 = slot_weights(found0)
    _, cells = gather_cells(places, inners, ens_copies)
    pl.semaphore_wait(barrier, n_lev + n_slab - 2)
    own_copies[0].wait()
    ring_begin(0)
    send_priors(0, cells, weights0)

    values0 = slot_values(found0)
    found1 = locate(1)
    places, inners = slot_places(found1)
    weights1 = slot_weights(found1)
    hot, now = gather_cells(places, inners)
    to_dev, to_gain = obs_order(found0)
    ring_forward(0)
    own_copies[1].wait()
    band_statistics(0, values0)
    for l in range(lev_rows):
        level_wide[l] = jnp.broadcast_to(column_of(found0, 7 + l), (n_obs, 128))
    ring_finish(0)

    weights = jnp.dot(loc_first[...].reshape(n_obs, cols), hot, preferred_element_type=F32)
    level_weight = jnp.zeros((n_obs, 128 * chunks), F32)
    for l in range(lev_rows):
        level_weight = jnp.where(inners == float(l), column_of(found0, 7 + l), level_weight)
    weights = level_weight * weights
    centred = (now - jnp.sum(now, axis=0, keepdims=True) / float(members)).astype(BF16)

    dev, gain = all_statistics(0, to_dev, to_gain)
    cross = jnp.dot(dev, centred, preferred_element_type=F32)
    mixed = (weights * cross).astype(BF16)
    now = now + jnp.dot(gain, mixed, preferred_element_type=F32)
    send_priors(1, now, weights1)
    ring_begin(1)

    crowd_out[0] = (jnp.maximum(found0[2], found1[2]) >= float(SLOTS * chunks)).astype(jnp.int32)
    mean_out[...] = mean_of(mean_rows(0), to_dev)
    values1 = slot_values(found1)
    regress(dev, gain)
    to_dev, to_gain = obs_order(found1)
    place_out[...] = to_dev
    ring_forward(1)
    band_statistics(1, values1)
    ring_finish(1)
    local = loc_last[...].reshape(n_obs, cols).astype(F32)
    for l in range(lev_rows):
        weight_out[l] = column_of(found1, 7 + l) * local
    dev, gain = all_statistics(1, to_dev, to_gain)
    dev_out[...] = dev
    gain_out[...] = gain
    packed_out[...] = mean_rows(1)
    remote.drain()


def run_filter(chunks, n_slab, n_lev, obs_cell, obs_value, obs_var, obs_frac, loc_level, ensemble, loc_column):
    members, lev_rows, cols = ensemble.shape
    n_obs = obs_cell.shape[1]
    held = loc_column.shape[1]
    width = WIDTH if cols % WIDTH == 0 else cols
    vmem = pl.BlockSpec(memory_space=pltpu.VMEM)
    hbm = pl.BlockSpec(memory_space=pltpu.HBM)
    dma = pltpu.SemaphoreType.DMA
    return pl.pallas_call(
        functools.partial(filter_kernel, chunks, n_slab, n_lev, width),
        out_shape=(
            pltpu.VMEM((lev_rows, members, cols), F32),
            pltpu.VMEM((lev_rows, members, cols), BF16),
            pltpu.VMEM((lev_rows, n_obs, cols), F32),
            pltpu.VMEM((n_obs, members), BF16),
            pltpu.VMEM((members, n_obs), BF16),
            pltpu.VMEM((n_obs, n_lev * chunks * 128), BF16),
            pltpu.VMEM((16, n_lev * chunks * 128), BF16),
            pltpu.VMEM((1, n_obs), F32),
            pltpu.SMEM((1,), jnp.int32),
        ),
        in_specs=[hbm] * 7,
        out_specs=(vmem,) * 8 + (pl.BlockSpec(memory_space=pltpu.SMEM),),
        scratch_shapes=[
            pltpu.VMEM((n_lev, held, cols), BF16),
            pltpu.VMEM((n_lev, held, cols), BF16),
            pltpu.VMEM(obs_cell.shape, jnp.int32),
            pltpu.VMEM(obs_cell.shape, F32),
            pltpu.VMEM(obs_cell.shape, F32),
            pltpu.VMEM(obs_cell.shape, F32),
            pltpu.VMEM(loc_level.shape, F32),
            pltpu.VMEM((2, n_slab, chunks, members // 2, 128), F32),
            pltpu.VMEM((2, n_lev, chunks, members + 16, 128), BF16),
            pltpu.VMEM((lev_rows, n_obs, 128), F32),
            dma((5,)),
            dma((lev_rows,)),
            dma((2,)),
            dma((2, n_slab)),
            dma((2, n_slab)),
            dma((2, n_lev)),
            dma((2, n_lev)),
            dma((2, 10)),
            dma((2, 10)),
        ],
        compiler_params=pltpu.CompilerParams(
            collective_id=chunks, has_side_effects=True, vmem_limit_bytes=VMEM_LIMIT
        ),
    )(*(pltpu.with_memory_space_constraint(x, pltpu.HBM) for x in (
        obs_cell, obs_value, obs_var, obs_frac, loc_level, ensemble, loc_column)))


def last_kernel(
    ens, centred, weight, dev_ref, gain_ref, place_ref, packed_ref, mean_ref,
    out_hbm, mean_hbm, out, mean, out_sem, mean_sem,
):
    lev_rows = ens.shape[0]
    dev = dev_ref[...]
    gain = gain_ref[...]
    copies = []
    for l in range(lev_rows):
        cross = jnp.dot(dev, centred[l], preferred_element_type=F32)
        mixed = (weight[l] * cross).astype(BF16)
        out[l] = ens[l] + jnp.dot(gain, mixed, preferred_element_type=F32)
        copies.append(pltpu.make_async_copy(out.at[l], out_hbm.at[:, l, :], out_sem.at[l]))
        copies[l].start()
        if l == MEAN_AFTER:
            mean[pl.ds(0, 1), :] = mean_ref[...]
            mean[pl.ds(1, 1), :] = mean_of(packed_ref[...], place_ref[...])
            mean_copy = pltpu.make_async_copy(mean, mean_hbm, mean_sem)
            mean_copy.start()
    for copy in copies:
        copy.wait()
    mean_copy.wait()


MEAN_AFTER = 3
PIECES = 2
VMEM_LIMIT = 40 * 1024 * 1024
WIDTH = 2304
COND = True


def last_update(ens, *rest):
    lev_rows, members, cols = ens.shape
    means = (2, rest[-1].shape[1])
    vmem = pl.BlockSpec(memory_space=pltpu.VMEM)
    hbm = pl.BlockSpec(memory_space=pltpu.HBM)
    return pl.pallas_call(
        last_kernel,
        out_shape=(pltpu.HBM((members, lev_rows, cols), F32), pltpu.HBM(means, F32)),
        in_specs=[vmem] * 8,
        out_specs=(hbm, hbm),
        scratch_shapes=[
            pltpu.VMEM((lev_rows, members, cols), F32),
            pltpu.VMEM(means, F32),
            pltpu.SemaphoreType.DMA((lev_rows,)),
            pltpu.SemaphoreType.DMA,
        ],
        compiler_params=pltpu.CompilerParams(vmem_limit_bytes=VMEM_LIMIT),
    )(*(pltpu.with_memory_space_constraint(x, pltpu.VMEM) for x in (ens, *rest)))


def on_device(n_slab, n_lev, ensemble, obs_cell, obs_value, obs_var, obs_frac, loc_column, loc_level):
    members, lev_rows, slab_cols = ensemble.shape
    n_obs = obs_cell.shape[1]
    operands = (obs_cell, obs_value, obs_var, obs_frac, jnp.swapaxes(loc_level, 1, 2), ensemble, loc_column)

    def whole(chunks):
        *state, crowd = run_filter(chunks, n_slab, n_lev, *operands)
        return (crowd[0], *last_update(*state))

    done = lax.while_loop(lambda state: state[0] != 0, lambda state: whole(3), whole(1))
    return done[1], done[2]


def solution(mesh):
    in_specs = (
        P(None, "lev", "slab"),
        P(),
        P(),
        P(),
        P(),
        P(None, "lev", "slab"),
        P(None, None, "lev"),
    )
    out_specs = (P(None, "lev", "slab"), P())
    return jax.shard_map(
        functools.partial(on_device, mesh.shape["slab"], mesh.shape["lev"]),
        mesh=mesh, in_specs=in_specs, out_specs=out_specs, check_vma=False,
    )
```

```python
import functools
import math

import jax
import jax.numpy as jnp
from jax import lax
from jax.experimental import pallas as pl
from jax.experimental.pallas import tpu as pltpu
from jax.sharding import PartitionSpec as P

MESH = pl.DeviceIdType.MESH
SLOTS = 64
F32 = jnp.float32
BF16 = jnp.bfloat16


def nt_dot(a, b):
    return lax.dot_general(a, b, (((1,), (1,)), ((), ())), preferred_element_type=F32)


def mean_of(packed, to_dev):
    parts = nt_dot(packed, to_dev)
    return parts[0:1] + parts[1:2] + parts[2:3]


def count_at_least(x, step, number):
    total = jnp.zeros_like(x)
    for k in range(1, number):
        total = total + jnp.where(x >= float(k * step), 1.0, 0.0)
    return total


def split3(x):
    high = x.astype(BF16)
    rest = x - high.astype(F32)
    mid = rest.astype(BF16)
    low = (rest - mid.astype(F32)).astype(BF16)
    return high, mid, low


class Tracker:
    def __init__(self):
        self.sends = []
        self.recvs = []

    def start(self, copy):
        copy.start()
        self.sends.append(copy)
        self.recvs.append(copy)

    def arrived(self, copy):
        copy.wait_recv()
        self.recvs = [c for c in self.recvs if c is not copy]

    def drain(self):
        for copy in self.recvs:
            copy.wait_recv()
        for copy in self.sends:
            copy.wait_send()


def filter_kernel(
    chunks, n_slab, n_lev, width,
    cell_hbm, value_hbm, var_hbm, frac_hbm, level_hbm, ens_hbm, loc_hbm,
    ens, centred_out, weight_out, dev_out, gain_out, place_out, packed_out, mean_out, crowd_out,
    loc_first, loc_last, cell_ref, value_ref, var_ref, frac_ref, level_ref, abuf, bbuf, level_wide,
    small_sem, ens_sem, own_sem, a_send, a_recv, b_send, b_recv, l_send, l_recv,
):
    slab = lax.axis_index("slab")
    lev = lax.axis_index("lev")
    lev_rows, members, cols = ens.shape
    n_obs = cell_ref.shape[1]
    loc = (loc_first, loc_last)
    total_cols = cols * n_slab
    half = members // 2
    remote = Tracker()

    barrier = pltpu.get_barrier_semaphore()
    side = math.isqrt(n_slab)
    stack = n_lev // 2

    def around(k, n):
        return min(k, n - k)

    slab_peer = [
        lax.rem(slab // side + k // side, side) * side + lax.rem(lax.rem(slab, side) + k % side, side)
        for k in range(n_slab)
    ]
    core = lax.rem(lev, 2)
    lev_peer = [
        lax.rem(lev // 2 + k // 2, stack) * 2 + (1 - core if k % 2 else core) for k in range(n_lev)
    ]
    slab_order = sorted(
        range(1, n_slab), key=lambda k: -around(k // side, side) - around(k % side, side)
    )
    lev_order = sorted(range(1, n_lev), key=lambda k: -around(k // 2, stack))
    small_copies = [
        pltpu.make_async_copy(source, target, small_sem.at[i])
        for i, (source, target) in enumerate([
            (cell_hbm, cell_ref), (value_hbm, value_ref), (var_hbm, var_ref),
            (frac_hbm, frac_ref), (level_hbm, level_ref),
        ])
    ]
    for copy in small_copies:
        copy.start()
    ens_copies = [
        pltpu.make_async_copy(ens_hbm.at[:, l, :], ens.at[l], ens_sem.at[l])
        for l in range(lev_rows)
    ]
    for copy in ens_copies:
        copy.start()
    for k in slab_order:
        pl.semaphore_signal(barrier, inc=1, device_id=(slab_peer[k], lev), device_id_type=MESH)
    for k in lev_order:
        pl.semaphore_signal(barrier, inc=1, device_id=(slab, lev_peer[k]), device_id_type=MESH)
    own_copies = [
        pltpu.make_async_copy(loc_hbm.at[b], loc[b].at[lev], own_sem.at[b]) for b in range(2)
    ]
    for copy in own_copies:
        copy.start()

    for copy in small_copies:
        copy.wait()

    slab_f = slab.astype(F32)
    lev_f = lev.astype(F32)
    lane = lax.broadcasted_iota(jnp.int32, (n_obs, 128), 1)
    lane_slot = jnp.where(lane < SLOTS, lane, lane - SLOTS).astype(F32)
    first_half = lane < SLOTS

    def locate(b):
        cell = cell_ref[pl.ds(b, 1), :].astype(F32)
        level = count_at_least(cell, total_cols, n_lev * lev_rows)
        column = cell - level * float(total_cols)
        later = column + 1.0
        later = jnp.where(later >= float(total_cols), 0.0, later)
        band = count_at_least(level, lev_rows, n_lev)
        inner = level - band * float(lev_rows)
        places = []
        for where_at in (column, later):
            in_slab = count_at_least(where_at, cols, n_slab)
            place = where_at - in_slab * float(cols) + 1.0
            places.append(jnp.where(in_slab == slab_f, place, 0.0))
        flat = [band, places[0], places[1], inner,
                value_ref[pl.ds(b, 1), :], var_ref[pl.ds(b, 1), :], frac_ref[pl.ds(b, 1), :]]
        flat = flat + [level_ref[b, pl.ds(l, 1), :] for l in range(lev_rows)]
        table = jnp.concatenate(flat + [jnp.zeros((128 - len(flat), n_obs), F32)], axis=0).T
        other = lax.broadcasted_iota(jnp.int32, (n_obs, n_obs), 1)
        mine = lax.broadcasted_iota(jnp.int32, (n_obs, n_obs), 0)
        earlier = (table[:, 0:1] == band) & (other < mine)
        rank = jnp.sum(jnp.where(earlier, 1.0, 0.0), axis=1, keepdims=True)
        return table, rank, jnp.max(rank)

    def column_of(found, i):
        return found[0][:, i : i + 1]

    def picked(found, q, x):
        chosen = (column_of(found, 0) == lev_f) & (found[1] == lane_slot + float(SLOTS * q))
        return jnp.sum(jnp.where(chosen, x, 0.0), axis=0, keepdims=True)

    def slot_places(found):
        place = jnp.where(first_half, column_of(found, 1), column_of(found, 2))
        inner = jnp.broadcast_to(column_of(found, 3), (n_obs, 128))
        return (
            jnp.concatenate([picked(found, q, place) - 1.0 for q in range(chunks)], axis=1),
            jnp.concatenate([picked(found, q, inner) for q in range(chunks)], axis=1),
        )

    def slot_weights(found):
        frac = column_of(found, 6)
        weight = jnp.where(first_half, 1.0 - frac, frac)
        return [picked(found, q, weight) for q in range(chunks)]

    def slot_values(found):
        pairs = []
        for q in range(chunks):
            value = picked(found, q, column_of(found, 4))
            var = picked(found, q, column_of(found, 5) - 1.0) + 1.0
            pairs.append((value, var))
        return pairs

    def gather_cells(places, inners, arriving=None):
        index = lax.broadcasted_iota(jnp.int32, (cols, 128 * chunks), 0).astype(F32)
        hot = jnp.where(index == places, 1.0, 0.0).astype(BF16)
        cells = jnp.zeros((members, 128 * chunks), F32)
        for l in range(lev_rows):
            if arriving is not None:
                arriving[l].wait()
            left = jnp.concatenate(split3(ens[l])[:PIECES], axis=0)
            found = jnp.dot(left, hot, preferred_element_type=F32)
            total = found[:members]
            for i in range(1, PIECES):
                total = total + found[i * members : (i + 1) * members]
            cells = jnp.where(inners == float(l), total, cells)
        return hot, jnp.where(places >= 0.0, cells, 0.0)

    def loc_copy(b, which, holder, start, count, target):
        piece = loc[b].at[holder, pl.ds(start, count)]
        return pltpu.make_async_remote_copy(
            src_ref=piece, dst_ref=piece,
            send_sem=l_send.at[b, which], recv_sem=l_recv.at[b, which],
            device_id=(slab, target), device_id_type=MESH,
        )

    up = lax.rem(lev + 2, n_lev)
    down = lax.rem(lev + n_lev - 2, n_lev)
    far = lax.rem(lev + 4, n_lev)
    mate = lev + 1 - 2 * lax.rem(lev, 2)
    held = loc_first.shape[1]
    part = held // 2
    ring = []
    for b in range(2):
        ring.append([
            loc_copy(b, 0, lev, 0, part, up),
            loc_copy(b, 1, lev, part, part, down),
            loc_copy(b, 2, lev, part, part, up),
            loc_copy(b, 3, lev, 0, part, down),
            loc_copy(b, 4, down, 0, part, up),
            loc_copy(b, 5, up, part, part, down),
            loc_copy(b, 6, lev, 0, held, mate),
            loc_copy(b, 7, down, 0, held, mate),
            loc_copy(b, 8, up, 0, held, mate),
            loc_copy(b, 9, far, 0, held, mate),
        ])

    def ring_begin(b):
        for i in (0, 1, 2, 3, 6):
            remote.start(ring[b][i])

    def ring_forward(b):
        for first, then in ((0, 4), (1, 5), (2, 7), (3, 8)):
            remote.arrived(ring[b][first])
            remote.start(ring[b][then])

    def ring_finish(b):
        remote.arrived(ring[b][4])
        remote.arrived(ring[b][5])
        remote.start(ring[b][9])
        for i in (6, 7, 8, 9):
            remote.arrived(ring[b][i])

    a_copies = [[
        pltpu.make_async_remote_copy(
            src_ref=abuf.at[r, 0], dst_ref=abuf.at[r, k],
            send_sem=a_send.at[r, k], recv_sem=a_recv.at[r, k],
            device_id=(slab_peer[k], lev), device_id_type=MESH,
        ) if k else None for k in range(n_slab)] for r in range(2)]
    b_copies = [[
        pltpu.make_async_remote_copy(
            src_ref=bbuf.at[r, 0], dst_ref=bbuf.at[r, k],
            send_sem=b_send.at[r, k], recv_sem=b_recv.at[r, k],
            device_id=(slab, lev_peer[k]), device_id_type=MESH,
        ) if k else None for k in range(n_lev)] for r in range(2)]

    lane1 = lax.broadcasted_iota(jnp.int32, (1, 128), 1)
    low1 = lane1 < SLOTS

    def send_priors(r, cells, weights):
        for q in range(chunks):
            weighted = cells[:, 128 * q : 128 * (q + 1)] * weights[q]
            both = weighted + pltpu.roll(weighted, SLOTS, 1)
            abuf[r, 0, q] = jnp.where(low1, both[:half], both[half:])
        for k in slab_order:
            remote.start(a_copies[r][k])

    def band_statistics(r, values):
        for k in range(1, n_slab):
            remote.arrived(a_copies[r][k])
        for q in range(chunks):
            packed = abuf[r, 0, q]
            for k in range(1, n_slab):
                packed = packed + abuf[r, k, q]
            turned = pltpu.roll(packed, SLOTS, 1)
            prior = jnp.concatenate(
                [jnp.where(low1, packed, turned), jnp.where(low1, turned, packed)], axis=0
            )
            value, variance = values[q]
            mean = jnp.sum(prior, axis=0, keepdims=True) / float(members)
            deviation = prior - mean
            spread = jnp.sum(deviation * deviation, axis=0, keepdims=True) / (members - 1.0)
            total = spread + variance
            shrink = 1.0 / (1.0 + jnp.sqrt(variance / total))
            gain = ((value - mean) - deviation * shrink) / (total * (members - 1.0))
            bbuf[r, 0, q, pl.ds(0, members), :] = jnp.where(low1, deviation, gain).astype(BF16)
            high, mid, low = (x.astype(F32) for x in split3(mean))
            row = lax.broadcasted_iota(jnp.int32, (16, 128), 0)
            parts = jnp.where(row == 0, high, jnp.where(row == 1, mid, jnp.where(row == 2, low, 0.0)))
            bbuf[r, 0, q, pl.ds(members, 16), :] = parts.astype(BF16)
        for k in lev_order:
            remote.start(b_copies[r][k])

    def obs_order(found):
        band = column_of(found, 0)
        band_stack = count_at_least(band, 2, stack)
        band_core = band - 2.0 * band_stack
        away = (lev // 2).astype(F32) - band_stack
        away = jnp.where(away < 0.0, away + float(stack), away) * 2.0
        away = away + jnp.where(band_core == core.astype(F32), 0.0, 1.0)
        to_dev = []
        to_gain = []
        for k in range(n_lev):
            for q in range(chunks):
                chosen = (away == float(k)) & (found[1] == lane_slot + float(SLOTS * q))
                to_dev.append(jnp.where(chosen & first_half, 1.0, 0.0).astype(BF16))
                to_gain.append(jnp.where(chosen & ~first_half, 1.0, 0.0).astype(BF16))
        return jnp.concatenate(to_dev, axis=1), jnp.concatenate(to_gain, axis=1)

    def all_statistics(r, to_dev, to_gain):
        for k in range(1, n_lev):
            remote.arrived(b_copies[r][k])
        packed = jnp.concatenate(
            [bbuf[r, k, q] for k in range(n_lev) for q in range(chunks)], axis=1
        )
        dev = nt_dot(to_dev, packed)[:, :members].astype(BF16)
        gain = nt_dot(packed[:members], to_gain).astype(BF16)
        return dev, gain

    def mean_rows(r):
        return jnp.concatenate(
            [bbuf[r, k, q, pl.ds(members, 16), :] for k in range(n_lev) for q in range(chunks)], axis=1
        )

    def at(c):
        return pl.ds(pl.multiple_of(c * width, width), width)

    def regress(dev, gain):
        def step(c, carry):
            local = loc_first[:, :, at(c)].reshape(n_obs, width).astype(F32)
            for l in range(lev_rows):
                now = ens[l, :, at(c)]
                mean = jnp.sum(now, axis=0, keepdims=True) / float(members)
                centred = (now - mean).astype(BF16)
                cross = jnp.dot(dev, centred, preferred_element_type=F32)
                weight = jnp.tile(level_wide[l], (1, width // 128)) * local
                mixed = (weight * cross).astype(BF16)
                now = now + jnp.dot(gain, mixed, preferred_element_type=F32)
                ens[l, :, at(c)] = now
                mean = jnp.sum(now, axis=0, keepdims=True) / float(members)
                centred_out[l, :, at(c)] = (now - mean).astype(BF16)
            return carry

        lax.fori_loop(0, cols // width, step, 0)

    found0 = locate(0)
    places, inners = slot_places(found0)
    weights0 = slot_weights(found0)
    _, cells = gather_cells(places, inners, ens_copies)
    pl.semaphore_wait(barrier, n_lev + n_slab - 2)
    send_priors(0, cells, weights0)
    own_copies[0].wait()
    ring_begin(0)

    values0 = slot_values(found0)
    found1 = locate(1)
    places, inners = slot_places(found1)
    weights1 = slot_weights(found1)
    hot, now = gather_cells(places, inners)
    to_dev, to_gain = obs_order(found0)
    ring_forward(0)
    own_copies[1].wait()
    band_statistics(0, values0)
    for l in range(lev_rows):
        level_wide[l] = jnp.broadcast_to(column_of(found0, 7 + l), (n_obs, 128))
    ring_finish(0)

    weights = jnp.dot(loc_first[...].reshape(n_obs, cols), hot, preferred_element_type=F32)
    level_weight = jnp.zeros((n_obs, 128 * chunks), F32)
    for l in range(lev_rows):
        level_weight = jnp.where(inners == float(l), column_of(found0, 7 + l), level_weight)
    weights = level_weight * weights
    centred = (now - jnp.sum(now, axis=0, keepdims=True) / float(members)).astype(BF16)

    dev, gain = all_statistics(0, to_dev, to_gain)
    cross = jnp.dot(dev, centred, preferred_element_type=F32)
    mixed = (weights * cross).astype(BF16)
    now = now + jnp.dot(gain, mixed, preferred_element_type=F32)
    send_priors(1, now, weights1)
    ring_begin(1)

    crowd_out[0] = (jnp.maximum(found0[2], found1[2]) >= float(SLOTS * chunks)).astype(jnp.int32)
    mean_out[...] = mean_of(mean_rows(0), to_dev)
    values1 = slot_values(found1)
    regress(dev, gain)
    to_dev, to_gain = obs_order(found1)
    place_out[...] = to_dev
    ring_forward(1)
    band_statistics(1, values1)
    ring_finish(1)
    local = loc_last[...].reshape(n_obs, cols).astype(F32)
    for l in range(lev_rows):
        weight_out[l] = column_of(found1, 7 + l) * local
    dev, gain = all_statistics(1, to_dev, to_gain)
    dev_out[...] = dev
    gain_out[...] = gain
    packed_out[...] = mean_rows(1)
    remote.drain()


def run_filter(chunks, n_slab, n_lev, obs_cell, obs_value, obs_var, obs_frac, loc_level, ensemble, loc_column):
    members, lev_rows, cols = ensemble.shape
    n_obs = obs_cell.shape[1]
    held = loc_column.shape[1]
    width = WIDTH if cols % WIDTH == 0 else cols
    vmem = pl.BlockSpec(memory_space=pltpu.VMEM)
    hbm = pl.BlockSpec(memory_space=pltpu.HBM)
    dma = pltpu.SemaphoreType.DMA
    return pl.pallas_call(
        functools.partial(filter_kernel, chunks, n_slab, n_lev, width),
        out_shape=(
            pltpu.VMEM((lev_rows, members, cols), F32),
            pltpu.VMEM((lev_rows, members, cols), BF16),
            pltpu.VMEM((lev_rows, n_obs, cols), F32),
            pltpu.VMEM((n_obs, members), BF16),
            pltpu.VMEM((members, n_obs), BF16),
            pltpu.VMEM((n_obs, n_lev * chunks * 128), BF16),
            pltpu.VMEM((16, n_lev * chunks * 128), BF16),
            pltpu.VMEM((1, n_obs), F32),
            pltpu.SMEM((1,), jnp.int32),
        ),
        in_specs=[hbm] * 7,
        out_specs=(vmem,) * 8 + (pl.BlockSpec(memory_space=pltpu.SMEM),),
        scratch_shapes=[
            pltpu.VMEM((n_lev, held, cols), BF16),
            pltpu.VMEM((n_lev, held, cols), BF16),
            pltpu.VMEM(obs_cell.shape, jnp.int32),
            pltpu.VMEM(obs_cell.shape, F32),
            pltpu.VMEM(obs_cell.shape, F32),
            pltpu.VMEM(obs_cell.shape, F32),
            pltpu.VMEM(loc_level.shape, F32),
            pltpu.VMEM((2, n_slab, chunks, members // 2, 128), F32),
            pltpu.VMEM((2, n_lev, chunks, members + 16, 128), BF16),
            pltpu.VMEM((lev_rows, n_obs, 128), F32),
            dma((5,)),
            dma((lev_rows,)),
            dma((2,)),
            dma((2, n_slab)),
            dma((2, n_slab)),
            dma((2, n_lev)),
            dma((2, n_lev)),
            dma((2, 10)),
            dma((2, 10)),
        ],
        compiler_params=pltpu.CompilerParams(
            collective_id=chunks, has_side_effects=True, vmem_limit_bytes=VMEM_LIMIT
        ),
    )(*(pltpu.with_memory_space_constraint(x, pltpu.HBM) for x in (
        obs_cell, obs_value, obs_var, obs_frac, loc_level, ensemble, loc_column)))


def last_kernel(
    ens, centred, weight, dev_ref, gain_ref, place_ref, packed_ref, mean_ref,
    out_hbm, mean_hbm, out, mean, out_sem, mean_sem,
):
    lev_rows = ens.shape[0]
    dev = dev_ref[...]
    gain = gain_ref[...]
    copies = []
    for l in range(lev_rows):
        cross = jnp.dot(dev, centred[l], preferred_element_type=F32)
        mixed = (weight[l] * cross).astype(BF16)
        out[l] = ens[l] + jnp.dot(gain, mixed, preferred_element_type=F32)
        copies.append(pltpu.make_async_copy(out.at[l], out_hbm.at[:, l, :], out_sem.at[l]))
        copies[l].start()
        if l == MEAN_AFTER:
            mean[pl.ds(0, 1), :] = mean_ref[...]
            mean[pl.ds(1, 1), :] = mean_of(packed_ref[...], place_ref[...])
            mean_copy = pltpu.make_async_copy(mean, mean_hbm, mean_sem)
            mean_copy.start()
    for copy in copies:
        copy.wait()
    mean_copy.wait()


MEAN_AFTER = 3
PIECES = 2
VMEM_LIMIT = 40 * 1024 * 1024
WIDTH = 2304
COND = True


def last_update(ens, *rest):
    lev_rows, members, cols = ens.shape
    means = (2, rest[-1].shape[1])
    vmem = pl.BlockSpec(memory_space=pltpu.VMEM)
    hbm = pl.BlockSpec(memory_space=pltpu.HBM)
    return pl.pallas_call(
        last_kernel,
        out_shape=(pltpu.HBM((members, lev_rows, cols), F32), pltpu.HBM(means, F32)),
        in_specs=[vmem] * 8,
        out_specs=(hbm, hbm),
        scratch_shapes=[
            pltpu.VMEM((lev_rows, members, cols), F32),
            pltpu.VMEM(means, F32),
            pltpu.SemaphoreType.DMA((lev_rows,)),
            pltpu.SemaphoreType.DMA,
        ],
        compiler_params=pltpu.CompilerParams(vmem_limit_bytes=VMEM_LIMIT),
    )(*(pltpu.with_memory_space_constraint(x, pltpu.VMEM) for x in (ens, *rest)))


def on_device(n_slab, n_lev, ensemble, obs_cell, obs_value, obs_var, obs_frac, loc_column, loc_level):
    members, lev_rows, slab_cols = ensemble.shape
    n_obs = obs_cell.shape[1]
    operands = (obs_cell, obs_value, obs_var, obs_frac, jnp.swapaxes(loc_level, 1, 2), ensemble, loc_column)

    def whole(chunks):
        *state, crowd = run_filter(chunks, n_slab, n_lev, *operands)
        return (crowd[0], *last_update(*state))

    done = lax.while_loop(lambda state: state[0] != 0, lambda state: whole(3), whole(1))
    return done[1], done[2]


def solution(mesh):
    in_specs = (
        P(None, "lev", "slab"),
        P(),
        P(),
        P(),
        P(),
        P(None, "lev", "slab"),
        P(None, None, "lev"),
    )
    out_specs = (P(None, "lev", "slab"), P())
    return jax.shard_map(
        functools.partial(on_device, mesh.shape["slab"], mesh.shape["lev"]),
        mesh=mesh, in_specs=in_specs, out_specs=out_specs, check_vma=False,
    )
```
